512 devices in a mesh: lat: 64 (over x, y, core), lev: 8 (over z).
Axes of the slice: x: 4, y: 8, z: 8, core: 2. Of those that a mesh axis runs over, the one named last changes fastest.
Arguments:
- anomalies: bfloat16 [4, 8, 80, 128, 1536], P(None, 'lev', None, 'lat'), may hold values from -6 to 6
- error_now: float32 [4, 8, 128, 1536], P(None, 'lev', 'lat'), may hold values from -6 to 6
- error_prior: float32 [4, 8, 128, 1536], P(None, 'lev', 'lat'), may hold values from -4.2 to 4.2
- energy_coef: float32 [4, 8], P(None, 'lev'), may hold values from 0.3 to 3
- obs_anomalies: bfloat16 [8192, 80, 256], P('lat', 'lev'), may hold values from -6 to 6
- innovations: float32 [8192, 256], P('lat'), may hold values from -6 to 6
- valid_counts: int32 [8192], P('lat'), may hold values from 0 to 256, as said below
- type_ids: int32 [8192], P('lat'), may hold values from 0 to 7
- error_inverse: float32 [8], replicated, may hold values from 0.25 to 4
Outputs:
- impact: float32 [8192, 16, 256], P('lat', 'lev')
- type_totals: float32 [16, 8], P('lev')
The draws below stay inside these ranges and needn't reach their ends.
Inputs may be any that keep to these rules, and one draw needn't show every extreme that they name: `valid_counts`: among the 128 slots of each index of lat, the blocks with a positive count come first and the first is always positive; in every draw some index of lat has all 128 slots positive and some block holds 256 rows. Rows below a block's count are observations, the rest padding.
All inputs are finite; a program needn't handle non-finite values.
Results may differ from the reference program's by a relative error of at most 0.0042.
Values may be sent and summed in bfloat16 or wider, within the bound.
A program may use at most 64 MiB of HBM per device.

```python
import math
import jax
import jax.numpy as jnp
from jax import lax

K = 80
NLON = 1536
NLAT_GRID = 768
LAT0 = 256
VARS = 4
REGIONS = 4
BLOCK = 256
NTYPES = 8
SLOTS = 128
NLAT = 128
NLEV = 8
NBLK = 8192
N_LAT = 64


def draw_valid_counts(key, part):
    key_list = jax.random.split(key, 5)
    first_draw = jax.random.randint(key_list[0], (N_LAT,), 1, SLOTS + 1)
    second = jax.random.randint(key_list[1], (N_LAT,), 1, SLOTS + 1)
    device_loads = jnp.maximum(first_draw * second // SLOTS, 1)
    busiest = jax.random.randint(key_list[2], (), 0, N_LAT)
    device_index = jnp.arange(N_LAT, dtype=jnp.int32)
    device_loads = jnp.where(device_index == busiest, SLOTS, device_loads)
    slot_index = jnp.arange(SLOTS, dtype=jnp.int32)
    rows_drawn = jax.random.randint(key_list[3], (N_LAT, SLOTS), 3 * BLOCK // 4, BLOCK + 1)
    fullest = jax.random.randint(key_list[4], (), 0, SLOTS)
    chosen = (device_index[:, None] == busiest) & (slot_index[None, :] == fullest)
    rows_drawn = jnp.where(chosen, BLOCK, rows_drawn)
    counts = jnp.where(slot_index[None, :] < device_loads[:, None], rows_drawn, 0)
    return counts.reshape(N_LAT * SLOTS).astype(jnp.int32)


def with_ends(result, rng, least, top_value):
    longest = result.shape.index(max(result.shape))
    spots = []
    for shift in (0, 1):
        where = [jax.random.randint(jax.random.fold_in(rng, axis), (), 0, length) for axis, length in enumerate(result.shape)]
        where[longest] = (where[longest] + shift) % result.shape[longest]
        spots.append(tuple(where))
    return result.at[spots[0]].set(least).at[spots[1]].set(top_value)


def shard_levels(key, shape, cuts, least, top_value):
    def one(position, parts):
        steps = jax.random.uniform(jax.random.fold_in(jax.random.fold_in(key, 6), position), (parts,), jnp.float32, least / len(cuts), top_value / len(cuts))
        return jnp.repeat(jnp.exp(steps), shape[position] // parts).reshape((-1,) + (1,) * (len(shape) - position - 1))

    gain = one(*cuts[0])
    for cut in cuts[1:]:
        gain = gain * one(*cut)
    return gain


def normal_values(rng, extent, scale, bound, shards=(), held_as=jnp.bfloat16):
    gain = shard_levels(rng, extent, shards, -0.22, 0.18) if shards else 1.0
    result = jax.random.normal(rng, extent, jnp.float32) * scale * gain
    return jnp.minimum(jnp.maximum(result, -bound), bound).astype(held_as)


def setup_inputs(seed: int = 0) -> dict:
    seeds = jax.random.split(jax.random.key(seed), 10)
    anomalies = normal_values(seeds[0], (VARS, NLEV, K, NLAT, NLON), 1.0, 6.0, ((1, 8), (3, 64)))
    error_now = normal_values(seeds[1], (VARS, NLEV, NLAT, NLON), 1.0, 6.0, ((1, 8), (2, 64)), jnp.float32)
    error_prior = normal_values(seeds[2], (VARS, NLEV, NLAT, NLON), 0.7, 4.2, ((1, 8), (2, 64)), jnp.float32)
    energy_coef = jnp.clip(jnp.exp(math.log(3.0) - 2.3025851 * jax.random.uniform(seeds[3], (VARS, NLEV), jnp.float32) ** shard_levels(seeds[3], (VARS, NLEV), ((1, 8),), -0.2, 0.2)), 0.3, 3.0)
    obs_anomalies = normal_values(seeds[4], (NBLK, K, BLOCK), 1.0, 6.0, ((0, 64), (1, 8)))
    innovations = normal_values(seeds[5], (NBLK, BLOCK), 1.0, 6.0, ((0, 64),), jnp.float32)
    valid_counts = draw_valid_counts(jax.random.fold_in(seeds[9], 71), 0)
    type_ids = with_ends(jax.random.randint(seeds[7], (NBLK,), 0, NTYPES), jax.random.fold_in(seeds[7], 1), 0, NTYPES - 1).astype(jnp.int32)
    error_inverse = jnp.clip(jnp.exp(jax.random.uniform(seeds[8], (NTYPES,), jnp.float32, math.log(0.25), math.log(4.0))), 0.25, 4.0)
    return {"anomalies": anomalies, "error_now": error_now, "error_prior": error_prior, "energy_coef": energy_coef, "obs_anomalies": obs_anomalies, "innovations": innovations, "valid_counts": valid_counts, "type_ids": type_ids, "error_inverse": error_inverse}


def reference(anomalies, error_now, error_prior, energy_coef, obs_anomalies, innovations, valid_counts, type_ids, error_inverse):
    lat_index = jnp.arange(NLAT, dtype=jnp.int32)
    cosine = jnp.cos(-0.5 * math.pi + ((lat_index + LAT0).astype(jnp.float32) + 0.5) * math.pi / NLAT_GRID)
    gradient = (energy_coef[:, :, None, None] * cosine[None, None, :, None] * (error_now + error_prior)).astype(jnp.bfloat16)

    def level_sum(running, level_id):
        level_block = lax.dynamic_index_in_dim(anomalies, level_id, 1, keepdims=False)
        level_grad = lax.dynamic_index_in_dim(gradient, level_id, 1, keepdims=False)
        folded = jnp.einsum('vkji,vji->vkj', level_block.astype(jnp.float32), level_grad.astype(jnp.float32))
        return (running + folded, None)
    folded_all, _ = lax.scan(level_sum, jnp.zeros((VARS, K, NLAT), jnp.float32), jnp.arange(NLEV, dtype=jnp.int32))
    region = lat_index * REGIONS // NLAT
    onehot = (region[None, :] == jnp.arange(REGIONS, dtype=jnp.int32)[:, None]).astype(jnp.float32)
    member_sums = jnp.einsum('vkj,rj->vkr', folded_all, onehot, precision=lax.Precision.HIGHEST)
    norm_scale = math.sqrt(NLEV * NLAT * NLON / REGIONS)
    weights = (jnp.transpose(member_sums, (1, 0, 2)).reshape(K, VARS * REGIONS) / norm_scale).astype(jnp.bfloat16)
    response = jnp.einsum('bks,kt->bts', obs_anomalies.astype(jnp.float32), weights.astype(jnp.float32))
    type_table = type_ids[:, None] == jnp.arange(NTYPES, dtype=jnp.int32)[None, :]
    inverse_var = lax.optimization_barrier(jnp.sum(jnp.where(type_table, error_inverse[None, :], jnp.zeros((), jnp.float32)), axis=1))
    positions = jnp.arange(BLOCK, dtype=jnp.int32)
    row_mask = (positions[None, :] < valid_counts[:, None]).astype(jnp.float32)
    scaling = innovations * inverse_var[:, None] * row_mask / math.sqrt(K - 1)
    impact = response * scaling[:, None, :]
    per_block = lax.optimization_barrier(jnp.sum(impact, axis=2))
    type_totals = jnp.dot(per_block.T, type_table.astype(jnp.float32), precision=lax.Precision.HIGHEST) / math.sqrt(NBLK * BLOCK / NTYPES)
    return (impact, type_totals)
```

```python
import functools
import math

import jax
import jax.numpy as jnp
from jax import lax
from jax.experimental import pallas as pl
from jax.experimental.pallas import tpu as pltpu
from jax.sharding import Mesh
from jax.sharding import PartitionSpec as P

NLAT_GRID = 768
LAT0 = 256
REGIONS = 4
NTYPES = 8
LAT = ("lat_0", "lat_1", "lat_2")
MESH = pl.DeviceIdType.MESH
F32 = jnp.float32
BF16 = jnp.bfloat16


def ring_order(n):
    return sorted(range(1, n), key=lambda d: (-min(d, n - d), d))


def exchange_kernel(
    dims,
    norm_scale,
    total_scale,
    part_ref,
    obs_v,
    scal_ref,
    type_ref,
    out_ref,
    tot_ref,
    mz,
    my,
    mx,
    mz_src,
    my_src,
    mx_src,
    obs_in,
    wd,
    resp_src,
    resp_in,
    pt_src,
    pt_in,
    mz_send,
    mz_recv,
    my_send,
    my_recv,
    mx_send,
    mx_recv,
    ob_send,
    ob_recv,
    rs_send,
    rs_recv,
    pt_send,
    pt_recv,
):
    nx, ny, nc, nz = dims
    members, slots, rows = obs_v.shape
    own = slots // nz
    targets = 16
    pair = targets // nz
    xi = lax.axis_index("lat_0")
    yi = lax.axis_index("lat_1")
    ci = lax.axis_index("lat_2")
    zi = lax.axis_index("lev")

    def z_peer(d):
        return {"lev": lax.rem(zi + d, nz)}

    def x_peer(d):
        return {"lat_0": lax.rem(xi + d, nx)}

    def y_peer(d, e):
        return {"lat_1": lax.rem(yi + d, ny), "lat_2": lax.rem(ci + e, nc)}

    y_steps = [(d, e) for d in ring_order(ny) + [0] for e in range(nc) if d or e]
    barrier = pltpu.get_barrier_semaphore()
    peers = [z_peer(d) for d in ring_order(nz)]
    peers += [y_peer(d, e) for d, e in y_steps]
    peers += [x_peer(d) for d in ring_order(nx)]
    for peer in peers:
        pl.semaphore_signal(barrier, inc=1, device_id=peer, device_id_type=MESH)

    onehot = (
        lax.broadcasted_iota(jnp.int32, (NTYPES, slots), 0) == type_ref[...]
    ).astype(F32)
    lane4 = lax.broadcasted_iota(jnp.int32, (4, 128), 1)
    payload = part_ref[...]
    base = payload
    g_add = jnp.zeros((4, 128), F32)
    scal = scal_ref[...]
    for m in range(members):
        prod = obs_v[m].astype(F32) * scal
        by_type = jnp.dot(
            onehot, prod, precision=lax.Precision.HIGHEST, preferred_element_type=F32
        )
        g = jnp.sum(by_type, axis=1, keepdims=True)
        g_add = jnp.where(lane4 == 80 + m, g[0:4], g_add)
        g_add = jnp.where(lane4 == 90 + m, g[4:8], g_add)
    mz_src[0] = base
    mz[pl.ds(zi, 1)] = base[None]

    mine = pl.ds(pl.multiple_of(zi * own, own), own)
    obs_in[pl.ds(zi, 1)] = obs_v[:, mine, :][None]

    pl.semaphore_wait(barrier, len(peers))

    z_copies = []
    for d in ring_order(nz):
        copy = pltpu.make_async_remote_copy(
            src_ref=mz_src.at[0],
            dst_ref=mz.at[zi],
            send_sem=mz_send.at[d],
            recv_sem=mz_recv.at[d],
            device_id=z_peer(d),
            device_id_type=MESH,
        )
        copy.start()
        z_copies.append(copy)
    ob_copies = []
    for d in ring_order(nz):
        other = lax.rem(zi + d, nz)
        there = pl.ds(pl.multiple_of(other * own, own), own)
        copy = pltpu.make_async_remote_copy(
            src_ref=obs_v.at[:, there, :],
            dst_ref=obs_in.at[zi],
            send_sem=ob_send.at[d],
            recv_sem=ob_recv.at[d],
            device_id=z_peer(d),
            device_id_type=MESH,
        )
        copy.start()
        ob_copies.append(copy)

    sel_cols = nz * members * own
    sel = (
        lax.broadcasted_iota(jnp.int32, (128, sel_cols), 0)
        == lax.broadcasted_iota(jnp.int32, (128, sel_cols), 1) // own
    ).astype(BF16)
    row_t = lax.broadcasted_iota(jnp.int32, (targets * own, targets), 0) // own
    col_t = lax.broadcasted_iota(jnp.int32, (targets * own, targets), 1)
    spread = (col_t == lax.rem(row_t, REGIONS) * 4 + row_t // REGIONS).astype(BF16)
    sel_z = (
        lax.broadcasted_iota(jnp.int32, (128, 128), 0)
        == lax.broadcasted_iota(jnp.int32, (128, 128), 1) + zi * members
    ) & (lax.broadcasted_iota(jnp.int32, (128, 128), 1) < members)
    sel_z = sel_z.astype(BF16)
    perm_r = lax.broadcasted_iota(jnp.int32, (targets, targets), 0)
    perm_c = lax.broadcasted_iota(jnp.int32, (targets, targets), 1)
    perm = (perm_c == lax.rem(perm_r, REGIONS) * 4 + perm_r // REGIONS).astype(BF16)

    for copy in z_copies:
        copy.wait()
    tot_z = mz[0]
    for z in range(1, nz):
        tot_z = tot_z + mz[z]
    tot_z = tot_z + g_add
    my_src[0] = tot_z
    here_y = yi * nc + ci
    my[pl.ds(here_y, 1)] = tot_z[None]
    y_copies = []
    for d, e in y_steps:
        copy = pltpu.make_async_remote_copy(
            src_ref=my_src.at[0],
            dst_ref=my.at[here_y],
            send_sem=my_send.at[d * nc + e],
            recv_sem=my_recv.at[d * nc + e],
            device_id=y_peer(d, e),
            device_id_type=MESH,
        )
        copy.start()
        y_copies.append(copy)
    for copy in y_copies:
        copy.wait()
    tot_y = my[0]
    for y in range(1, ny * nc):
        tot_y = tot_y + my[y]
    mx_src[0] = tot_y
    mx[pl.ds(xi, 1)] = tot_y[None]
    x_copies = []
    for d in ring_order(nx):
        copy = pltpu.make_async_remote_copy(
            src_ref=mx_src.at[0],
            dst_ref=mx.at[xi],
            send_sem=mx_send.at[d],
            recv_sem=mx_recv.at[d],
            device_id=x_peer(d),
            device_id_type=MESH,
        )
        copy.start()
        x_copies.append(copy)
    for copy in x_copies:
        copy.wait()

    sums = jnp.concatenate([mx[x] for x in range(nx)], axis=0)
    lane16 = lax.broadcasted_iota(jnp.int32, (targets, 128), 1)
    w = jnp.where(lane16 < 80, sums / norm_scale, 0.0).astype(BF16)
    g_all = mx[0]
    for x in range(1, nx):
        g_all = g_all + mx[x]

    wide = jnp.dot(w, sel, preferred_element_type=F32).astype(BF16)
    tall = jnp.dot(spread, wide, preferred_element_type=F32)
    shape = (targets * own, sel_cols)
    keep = lax.rem(lax.broadcasted_iota(jnp.int32, shape, 0), own) == lax.rem(
        lax.broadcasted_iota(jnp.int32, shape, 1), own
    )
    wd[...] = jnp.where(keep, tall, 0.0).astype(BF16)

    for copy in ob_copies:
        copy.wait()
    gathered = obs_in[...].reshape(sel_cols, rows)
    answered = jnp.dot(wd[...], gathered, preferred_element_type=F32)
    resp_src[...] = answered.astype(BF16).reshape(nz, pair, own, rows)
    rs_copies = []
    for d in ring_order(nz):
        other = lax.rem(zi + d, nz)
        copy = pltpu.make_async_remote_copy(
            src_ref=resp_src.at[other],
            dst_ref=resp_in.at[zi],
            send_sem=rs_send.at[d],
            recv_sem=rs_recv.at[d],
            device_id=z_peer(d),
            device_id_type=MESH,
        )
        copy.start()
        rs_copies.append(copy)
    resp_in[pl.ds(zi, 1)] = resp_src[pl.ds(zi, 1)]

    w_own = jnp.dot(w, sel_z, preferred_element_type=F32).astype(BF16)
    w_own = jnp.dot(perm, w_own, preferred_element_type=F32)
    g_low = pltpu.roll(g_all, 128 - 80, 1)
    g_high = pltpu.roll(g_all, 128 - 90, 1)
    g_rows = jnp.concatenate([g_low, g_high], axis=0)
    lane8 = lax.broadcasted_iota(jnp.int32, (NTYPES, 128), 1)
    g_rows = jnp.where(lane8 < members, g_rows, 0.0)
    lanes = lax.broadcasted_iota(jnp.int32, (targets, 128), 1)
    share = jnp.zeros((targets, 128), F32)
    for c in range(NTYPES):
        col = jnp.sum(w_own * g_rows[c : c + 1], axis=1, keepdims=True)
        share = jnp.where(lanes == c, col, share)
    for z in range(nz):
        pt_src[z, 0:pair, :] = share[pair * z : pair * z + pair]
    pt_copies = []
    for d in ring_order(nz):
        other = lax.rem(zi + d, nz)
        copy = pltpu.make_async_remote_copy(
            src_ref=pt_src.at[other, pl.ds(0, pair)],
            dst_ref=pt_in.at[zi, pl.ds(0, pair)],
            send_sem=pt_send.at[d],
            recv_sem=pt_recv.at[d],
            device_id=z_peer(d),
            device_id_type=MESH,
        )
        copy.start()
        pt_copies.append(copy)
    pt_in[pl.ds(zi, 1), 0:pair, :] = pt_src[pl.ds(zi, 1), 0:pair, :]

    for copy in rs_copies:
        copy.wait()
    for z in range(nz):
        for t in range(pair):
            value = resp_in[z, t].astype(F32) * scal_ref[z * own : (z + 1) * own, :]
            for half in range(2):
                out_ref[pl.ds(z * own * 4 + half * 2 + t, own, stride=4), :] = value[
                    :, half * 128 : (half + 1) * 128
                ]
    for copy in pt_copies:
        copy.wait()
    whole = pt_in[0, 0:pair, :]
    for z in range(1, nz):
        whole = whole + pt_in[z, 0:pair, :]
    tot_ref[...] = whole[:, 0:NTYPES] / total_scale


def local(
    anomalies,
    error_now,
    error_prior,
    energy_coef,
    obs_anomalies,
    innovations,
    valid_counts,
    type_ids,
    error_inverse,
):
    dims = tuple(lax.axis_size(a) for a in (*LAT, "lev"))
    lat_rows = error_now.shape[2]
    lat_total = lat_rows * lax.axis_size(LAT)
    lev_total = error_now.shape[1] * lax.axis_size("lev")
    lon_count = error_now.shape[3]
    lat_index = lax.axis_index(LAT) * lat_rows + jnp.arange(lat_rows, dtype=jnp.int32)
    cosine = jnp.cos(
        -0.5 * math.pi + ((lat_index + LAT0).astype(F32) + 0.5) * math.pi / NLAT_GRID
    )
    gradient = (
        energy_coef[:, :, None, None] * cosine[None, None, :, None] * (error_now + error_prior)
    ).astype(BF16)
    folded = jnp.einsum("vlkji,vlji->vk", anomalies, gradient, preferred_element_type=F32)
    members = anomalies.shape[2]
    variables = anomalies.shape[0]
    part = jnp.pad(folded, ((0, 0), (0, 128 - members)))
    norm_scale = math.sqrt(lev_total * lat_total * lon_count / REGIONS)
    slots, local_members, rows = obs_anomalies.shape
    type_table = type_ids[:, None] == jnp.arange(NTYPES, dtype=jnp.int32)[None, :]
    inverse_var = jnp.sum(
        jnp.where(type_table, error_inverse[None, :], jnp.zeros((), F32)), axis=1
    )
    positions = jnp.arange(rows, dtype=jnp.int32)
    row_mask = (positions[None, :] < valid_counts[:, None]).astype(F32)
    scaling = innovations * inverse_var[:, None] * row_mask / math.sqrt(members - 1)
    total_scale = math.sqrt(slots * lax.axis_size(LAT) * rows / NTYPES)
    nx, ny, nc, nz = dims
    own = slots // nz
    targets = variables * REGIONS
    pair = targets // nz
    vmem = pl.BlockSpec(memory_space=pltpu.VMEM)
    dma = pltpu.SemaphoreType.DMA
    out, totals = pl.pallas_call(
        functools.partial(exchange_kernel, dims, norm_scale, total_scale),
        out_shape=(
            jax.ShapeDtypeStruct((slots * pair * rows // 128, 128), F32),
            jax.ShapeDtypeStruct((pair, NTYPES), F32),
        ),
        in_specs=[vmem, vmem, vmem, vmem],
        out_specs=(vmem, vmem),
        scratch_shapes=[
            pltpu.VMEM((nz, 4, 128), F32),
            pltpu.VMEM((ny * nc, 4, 128), F32),
            pltpu.VMEM((nx, 4, 128), F32),
            pltpu.VMEM((1, 4, 128), F32),
            pltpu.VMEM((1, 4, 128), F32),
            pltpu.VMEM((1, 4, 128), F32),
            pltpu.VMEM((nz, local_members, own, rows), BF16),
            pltpu.VMEM((targets * own, nz * local_members * own), BF16),
            pltpu.VMEM((nz, pair, own, rows), BF16),
            pltpu.VMEM((nz, pair, own, rows), BF16),
            pltpu.VMEM((nz, 8, 128), F32),
            pltpu.VMEM((nz, 8, 128), F32),
            dma((nz,)),
            dma((nz,)),
            dma((ny * nc,)),
            dma((ny * nc,)),
            dma((nx,)),
            dma((nx,)),
            dma((nz,)),
            dma((nz,)),
            dma((nz,)),
            dma((nz,)),
            dma((nz,)),
            dma((nz,)),
        ],
        compiler_params=pltpu.CompilerParams(
            collective_id=0, has_side_effects=True, vmem_limit_bytes=32 * 1024 * 1024
        ),
    )(part, jnp.transpose(obs_anomalies, (1, 0, 2)), scaling, type_ids.reshape(1, slots))
    impact = out.reshape(slots, rows // 128, pair, 128)
    impact = jnp.transpose(impact, (0, 2, 1, 3)).reshape(slots, pair, rows)
    return (impact, totals)


def solution(mesh):
    split = Mesh(
        mesh.devices.reshape(4, 8, 2, mesh.shape["lev"]), ("lat_0", "lat_1", "lat_2", "lev")
    )
    in_specs = (
        P(None, "lev", None, LAT, None),
        P(None, "lev", LAT, None),
        P(None, "lev", LAT, None),
        P(None, "lev"),
        P(LAT, "lev", None),
        P(LAT, None),
        P(LAT),
        P(LAT),
        P(),
    )
    out_specs = (P(LAT, "lev", None), P("lev", None))
    return jax.shard_map(local, mesh=split, in_specs=in_specs, out_specs=out_specs, check_vma=False)
```

```python
import functools
import math

import jax
import jax.numpy as jnp
from jax import lax
from jax.experimental.layout import Layout, with_layout_constraint
from jax.experimental import pallas as pl
from jax.experimental.pallas import tpu as pltpu
from jax.sharding import Mesh
from jax.sharding import PartitionSpec as P

NLAT_GRID = 768
LAT0 = 256
REGIONS = 4
NTYPES = 8
LAT = ("lat_0", "lat_1", "lat_2")
MESH = pl.DeviceIdType.MESH
F32 = jnp.float32
BF16 = jnp.bfloat16


def ring_order(n):
    return sorted(range(1, n), key=lambda d: (-min(d, n - d), d))


def exchange_kernel(
    dims,
    counts,
    norm_scale,
    member_scale,
    total_scale,
    anom_ref,
    now_ref,
    prior_ref,
    energy_ref,
    obs_ref,
    innov_ref,
    valid_ref,
    type_ref,
    inverse_ref,
    out_ref,
    tot_ref,
    anom,
    now,
    prior,
    energy,
    obs,
    innov,
    valid,
    types,
    inverse,
    folded,
    scal,
    mz,
    my,
    mx,
    mz_src,
    my_src,
    mx_src,
    near,
    far_up,
    far_down,
    resp_src,
    resp_in,
    pt_src,
    pt_in,
    load_sem,
    mz_send,
    mz_recv,
    my_send,
    my_recv,
    mx_send,
    mx_recv,
    ob_send,
    ob_recv,
    rs_send,
    rs_recv,
    pt_send,
    pt_recv,
):
    nx, ny, nc, nz = dims
    variables, total_members, lat_rows = counts
    members, slots, rows = obs.shape
    owners = nz // 2
    block = slots // owners
    half = block // 2
    targets = variables * REGIONS
    pair = targets // nz
    lon_tiles = now.shape[1]
    xi = lax.axis_index("lat_0")
    yi = lax.axis_index("lat_1")
    ci = lax.axis_index("lat_2")
    zi = lax.axis_index("lev")

    def loads(pairs, first):
        copies = []
        for i, (a, b) in enumerate(pairs):
            copy = pltpu.make_async_copy(a, b, load_sem.at[first + i])
            copy.start()
            copies.append(copy)
        return copies

    grad_loads = loads([(now_ref, now), (prior_ref, prior), (energy_ref, energy)], 0)
    anom_loads = loads([(anom_ref.at[v], anom.at[v]) for v in range(variables)], 3)

    def z_peer(d):
        return {"lev": lax.rem(zi + d, nz)}

    def x_peer(d):
        return {"lat_0": lax.rem(xi + d, nx)}

    def y_peer(d, e):
        return {"lat_1": lax.rem(yi + d, ny), "lat_2": lax.rem(ci + e, nc)}

    def send(source, target, sems, d, peer):
        copy = pltpu.make_async_remote_copy(
            src_ref=source,
            dst_ref=target,
            send_sem=sems[0].at[d],
            recv_sem=sems[1].at[d],
            device_id=peer,
            device_id_type=MESH,
        )
        copy.start()
        return copy

    def iota(shape, axis):
        return lax.broadcasted_iota(jnp.int32, shape, axis)

    y_steps = [(d, e) for d in ring_order(ny) + [0] for e in range(nc) if d or e]
    barrier = pltpu.get_barrier_semaphore()
    peers = [z_peer(d) for d in ring_order(nz)]
    peers += [y_peer(d, e) for d, e in y_steps]
    peers += [x_peer(d) for d in ring_order(nx)]
    for peer in peers:
        pl.semaphore_signal(barrier, inc=1, device_id=peer, device_id_type=MESH)
    other_loads = loads(
        [
            (obs_ref, obs),
            (innov_ref, innov),
            (valid_ref, valid),
            (type_ref, types),
            (inverse_ref, inverse),
        ],
        3 + variables,
    )

    lat_index = ((xi * ny + yi) * nc + ci) * lat_rows + lax.rem(
        iota((lon_tiles, 128), 0), lat_rows
    )
    cosine = jnp.cos(
        -0.5 * math.pi + ((lat_index + LAT0).astype(F32) + 0.5) * math.pi / NLAT_GRID
    )
    for copy in grad_loads:
        copy.wait()
    spare = jnp.zeros((128 - total_members, 384), BF16)
    for v in range(variables):
        grad = energy[0:1, v : v + 1] * cosine * (now[v] + prior[v])
        grad = grad.astype(BF16).astype(F32)
        anom_loads[v].wait()
        step = 4
        for k in range(0, anom.shape[1], step):
            a = anom[v, k : k + step].astype(F32)
            a = a.reshape(-1, lon_tiles, 128) * grad[None]
            a = a.reshape(a.shape[0], lon_tiles // 8, 8, 128).sum(axis=1)
            folded[v, k * 16 : (k + step) * 16, :] = a.reshape(-1, 128)
    lines = []
    for v in range(variables):
        s = folded[v, pl.ds(0, total_members, stride=8), :]
        for r in range(1, 8):
            s = s + folded[v, pl.ds(r, total_members, stride=8), :]
        high = s.astype(BF16)
        rest = s - high.astype(F32)
        mid = rest.astype(BF16)
        low = (rest - mid.astype(F32)).astype(BF16)
        lines.append(
            jnp.concatenate([jnp.concatenate([high, mid, low], axis=1), spare], axis=0)
        )
    lanes_sum = lax.dot_general(
        jnp.ones((8, 384), BF16),
        jnp.concatenate(lines, axis=0),
        (((1,), (1,)), ((), ())),
        preferred_element_type=F32,
    )
    row4 = iota((4, 128), 0)
    lane4 = iota((4, 128), 1)
    base = jnp.zeros((4, 128), F32)
    for v in range(variables):
        base = jnp.where(row4 == v, lanes_sum[0:4, v * 128 : (v + 1) * 128], base)
    mz_src[0] = base
    mz[pl.ds(zi, 1)] = base[None]

    pl.semaphore_wait(barrier, len(peers))
    z_copies = [
        send(mz_src.at[0], mz.at[zi], (mz_send, mz_recv), d, z_peer(d))
        for d in ring_order(nz)
    ]

    for copy in other_loads:
        copy.wait()
    eye = iota((slots, slots), 0) == iota((slots, slots), 1)

    def column(line):
        wide = jnp.broadcast_to(line.astype(F32), (slots, slots))
        return jnp.sum(jnp.where(eye, wide, 0.0), axis=1, keepdims=True)

    type_col = column(types[...])
    valid_col = column(valid[...])
    inverse_col = jnp.zeros((slots, 1), F32)
    for c in range(NTYPES):
        inverse_col = jnp.where(type_col == c, inverse[0:1, c : c + 1], inverse_col)
    inside = iota((slots, rows), 1).astype(F32) < valid_col
    scaled = innov[...] * inverse_col * inside.astype(F32) / member_scale
    scal[...] = scaled
    onehot = (iota((NTYPES, slots), 0) == types[...]).astype(F32)
    g_add = jnp.zeros((4, 128), F32)
    for m in range(members):
        prod = obs[m].astype(F32) * scal[...]
        by_type = jnp.dot(
            onehot, prod, precision=lax.Precision.HIGHEST, preferred_element_type=F32
        )
        g = jnp.sum(by_type, axis=1, keepdims=True)
        g_add = jnp.where(lane4 == total_members + m, g[0:4], g_add)
        g_add = jnp.where(lane4 == total_members + members + m, g[4:8], g_add)
    my_class = lax.rem(zi, owners)
    mine = pl.ds(pl.multiple_of(my_class * block, block), block)
    near[1] = obs[:, mine, :]

    def select(cols, first):
        wanted = lax.rem(
            zi * members + (first * members + 2 * total_members) + iota((128, cols), 1) // half,
            total_members,
        )
        return (iota((128, cols), 0) == wanted).astype(BF16)

    one = members * half
    sel_near = select(3 * one, -1)
    sel_up = select(one, 2)
    sel_down = select(one, -2)
    row_t = iota((targets * half, targets), 0) // half
    spread = (
        iota((targets * half, targets), 1)
        == lax.rem(row_t, REGIONS) * variables + row_t // REGIONS
    ).astype(BF16)
    sel_own = (
        (iota((128, 128), 0) == iota((128, 128), 1) + zi * members)
        & (iota((128, 128), 1) < members)
    ).astype(BF16)
    perm_r = iota((targets, targets), 0)
    perm = (
        iota((targets, targets), 1) == lax.rem(perm_r, REGIONS) * variables + perm_r // REGIONS
    ).astype(BF16)

    for copy in z_copies:
        copy.wait()
    tot_z = mz[0]
    for z in range(1, nz):
        tot_z = tot_z + mz[z]
    tot_z = tot_z + g_add
    my_src[0] = tot_z
    here_y = yi * nc + ci
    my[pl.ds(here_y, 1)] = tot_z[None]
    y_copies = [
        send(my_src.at[0], my.at[here_y], (my_send, my_recv), d * nc + e, y_peer(d, e))
        for d, e in y_steps
    ]

    def class_at(d, first, size):
        c = lax.rem(zi + d, owners)
        return pl.ds(pl.multiple_of(c * block + first, half), size)

    sems = (ob_send, ob_recv)
    ob_copies = [
        send(obs.at[:, class_at(2, half, half), :], far_down, sems, 0, z_peer(2)),
        send(obs.at[:, class_at(nz - 2, 0, half), :], far_up, sems, 1, z_peer(nz - 2)),
        send(obs.at[:, class_at(1, 0, block), :], near.at[0], sems, 2, z_peer(1)),
        send(obs.at[:, class_at(nz - 1, 0, block), :], near.at[2], sems, 3, z_peer(nz - 1)),
    ]

    for copy in y_copies:
        copy.wait()
    tot_y = my[0]
    for y in range(1, ny * nc):
        tot_y = tot_y + my[y]
    mx_src[0] = tot_y
    mx[pl.ds(xi, 1)] = tot_y[None]
    x_copies = [
        send(mx_src.at[0], mx.at[xi], (mx_send, mx_recv), d, x_peer(d))
        for d in ring_order(nx)
    ]
    for copy in x_copies:
        copy.wait()

    sums = jnp.concatenate([mx[x] for x in range(nx)], axis=0)
    lane16 = iota((targets, 128), 1)
    w = jnp.where(lane16 < total_members, sums / norm_scale, 0.0).astype(BF16)
    g_all = mx[0]
    for x in range(1, nx):
        g_all = g_all + mx[x]

    def diagonal(sel):
        wide = jnp.dot(w, sel, preferred_element_type=F32).astype(BF16)
        tall = jnp.dot(spread, wide, preferred_element_type=F32)
        keep = lax.rem(iota(tall.shape, 0), half) == lax.rem(iota(tall.shape, 1), half)
        return jnp.where(keep, tall, 0.0).astype(BF16)

    wd_near = diagonal(sel_near)
    wd_up = diagonal(sel_up)
    wd_down = diagonal(sel_down)

    w_own = jnp.dot(w, sel_own, preferred_element_type=F32).astype(BF16)
    w_own = jnp.dot(perm, w_own, preferred_element_type=F32)
    g_rows = jnp.concatenate(
        [
            pltpu.roll(g_all, 128 - total_members, 1),
            pltpu.roll(g_all, 128 - total_members - members, 1),
        ],
        axis=0,
    )
    g_rows = jnp.where(iota((NTYPES, 128), 1) < members, g_rows, 0.0)
    share = jnp.zeros((targets, 128), F32)
    for c in range(NTYPES):
        col = jnp.sum(w_own * g_rows[c : c + 1], axis=1, keepdims=True)
        share = jnp.where(lane16 == c, col, share)
    for z in range(nz):
        pt_src[z, 0:pair, :] = share[pair * z : pair * z + pair]
    top = pl.ds(0, pair)
    pt_copies = [
        send(
            pt_src.at[lax.rem(zi + d, nz), top],
            pt_in.at[zi, top],
            (pt_send, pt_recv),
            d,
            z_peer(d),
        )
        for d in ring_order(nz)
    ]
    pt_in[pl.ds(zi, 1), 0:pair, :] = pt_src[pl.ds(zi, 1), 0:pair, :]

    for copy in ob_copies:
        copy.wait()
    rs_copies = []
    for g, (wd_far, far) in enumerate(((wd_up, far_up), (wd_down, far_down))):
        part = pl.ds(g * half, half)
        close = near[:, :, g * half : (g + 1) * half, :].reshape(3 * one, rows)
        answered = jnp.dot(wd_near, close, preferred_element_type=F32)
        answered += jnp.dot(
            wd_far, far[...].reshape(one, rows), preferred_element_type=F32
        )
        resp_src[:, g] = answered.astype(BF16).reshape(nz, pair, half, rows)
        for d in ring_order(nz):
            rs_copies.append(
                send(
                    resp_src.at[lax.rem(zi + d, nz), g],
                    resp_in.at[zi, g],
                    (rs_send, rs_recv),
                    g * nz + d,
                    z_peer(d),
                )
            )
    resp_in[pl.ds(zi, 1)] = resp_src[pl.ds(zi, 1)]

    for copy in rs_copies:
        copy.wait()
    for c in range(owners):
        for g in range(2):
            first = c * block + g * half
            for t in range(pair):
                value = resp_in[c, g, t].astype(F32) + resp_in[c + owners, g, t].astype(F32)
                value = value * scal[first : first + half, :]
                for lane in range(rows // 128):
                    place = (first * (rows // 128) + lane) * pair + t
                    out_ref[pl.ds(place, half, stride=pair * (rows // 128)), :] = value[
                        :, lane * 128 : (lane + 1) * 128
                    ]
    for copy in pt_copies:
        copy.wait()
    whole = pt_in[0, 0:pair, :]
    for z in range(1, nz):
        whole = whole + pt_in[z, 0:pair, :]
    tot_ref[...] = whole[:, 0:NTYPES] / total_scale


def local(
    anomalies,
    error_now,
    error_prior,
    energy_coef,
    obs_anomalies,
    innovations,
    valid_counts,
    type_ids,
    error_inverse,
):
    dims = tuple(lax.axis_size(a) for a in (*LAT, "lev"))
    nx, ny, nc, nz = dims
    variables, levels, members, lat_rows, lon_count = anomalies.shape
    slots, local_members, rows = obs_anomalies.shape
    lat_total = lat_rows * nx * ny * nc
    norm_scale = math.sqrt(levels * nz * lat_total * lon_count / REGIONS)
    member_scale = math.sqrt(members - 1)
    total_scale = math.sqrt(slots * nx * ny * nc * rows / NTYPES)
    targets = variables * REGIONS
    pair = targets // nz
    block = slots // (nz // 2)
    half = block // 2
    tiles = lon_count // 128 * lat_rows

    def by_tile(a):
        a = a.reshape(*a.shape[:-1], lon_count // 128, 128)
        n = a.ndim
        order = (*range(n - 3), n - 2, n - 3, n - 1)
        a = with_layout_constraint(a, Layout(major_to_minor=order))
        a = jnp.swapaxes(a, -3, -2)
        return a.reshape(*a.shape[:-3], tiles, 128)

    anom = by_tile(anomalies[:, 0]).reshape(variables, members // 2, 2 * tiles, 128)
    now = by_tile(error_now[:, 0])
    prior = by_tile(error_prior[:, 0])
    obs = jnp.transpose(obs_anomalies, (1, 0, 2))
    inputs = (
        anom,
        now,
        prior,
        energy_coef.reshape(1, variables),
        obs,
        innovations,
        valid_counts.reshape(1, slots),
        type_ids.reshape(1, slots),
        error_inverse.reshape(1, NTYPES),
    )
    vmem = pl.BlockSpec(memory_space=pltpu.VMEM)
    hbm = pl.BlockSpec(memory_space=pltpu.HBM)
    dma = pltpu.SemaphoreType.DMA
    table = pltpu.VMEM
    out, totals = pl.pallas_call(
        functools.partial(
            exchange_kernel,
            dims,
            (variables, members, lat_rows),
            norm_scale,
            member_scale,
            total_scale,
        ),
        out_shape=(
            jax.ShapeDtypeStruct((slots * pair * rows // 128, 128), F32),
            jax.ShapeDtypeStruct((pair, NTYPES), F32),
        ),
        in_specs=[hbm] * len(inputs),
        out_specs=(vmem, vmem),
        scratch_shapes=[table(a.shape, a.dtype) for a in inputs]
        + [
            table((variables, members * 8, 128), F32),
            table((slots, rows), F32),
            table((nz, 4, 128), F32),
            table((ny * nc, 4, 128), F32),
            table((nx, 4, 128), F32),
            table((1, 4, 128), F32),
            table((1, 4, 128), F32),
            table((1, 4, 128), F32),
            table((3, local_members, block, rows), BF16),
            table((local_members, half, rows), BF16),
            table((local_members, half, rows), BF16),
            table((nz, 2, pair, half, rows), BF16),
            table((nz, 2, pair, half, rows), BF16),
            table((nz, 8, 128), F32),
            table((nz, 8, 128), F32),
            dma((8 + variables,)),
            dma((nz,)),
            dma((nz,)),
            dma((ny * nc,)),
            dma((ny * nc,)),
            dma((nx,)),
            dma((nx,)),
            dma((4,)),
            dma((4,)),
            dma((2 * nz,)),
            dma((2 * nz,)),
            dma((nz,)),
            dma((nz,)),
        ],
        compiler_params=pltpu.CompilerParams(
            collective_id=0, has_side_effects=True, vmem_limit_bytes=24 * 1024 * 1024
        ),
    )(*inputs)
    impact = out.reshape(slots, rows // 128, pair, 128)
    impact = jnp.transpose(impact, (0, 2, 1, 3)).reshape(slots, pair, rows)
    return (impact, totals)


def solution(mesh):
    split = Mesh(
        mesh.devices.reshape(4, 8, 2, mesh.shape["lev"]), ("lat_0", "lat_1", "lat_2", "lev")
    )
    in_specs = (
        P(None, "lev", None, LAT, None),
        P(None, "lev", LAT, None),
        P(None, "lev", LAT, None),
        P(None, "lev"),
        P(LAT, "lev", None),
        P(LAT, None),
        P(LAT),
        P(LAT),
        P(),
    )
    out_specs = (P(LAT, "lev", None), P("lev", None))
    return jax.shard_map(local, mesh=split, in_specs=in_specs, out_specs=out_specs, check_vma=False)
```

```python
import functools
import math

import jax
import jax.numpy as jnp
from jax import lax
from jax.experimental.layout import Layout, with_layout_constraint
from jax.experimental import pallas as pl
from jax.experimental.pallas import tpu as pltpu
from jax.sharding import Mesh
from jax.sharding import PartitionSpec as P

NLAT_GRID = 768
LAT0 = 256
REGIONS = 4
NTYPES = 8
LAT = ("lat_0", "lat_1", "lat_2")
MESH = pl.DeviceIdType.MESH
F32 = jnp.float32
BF16 = jnp.bfloat16


def ring_order(n):
    return sorted(range(1, n), key=lambda d: (-min(d, n - d), d))


def exchange_kernel(
    dims,
    counts,
    norm_scale,
    member_scale,
    total_scale,
    anom_ref,
    now_ref,
    prior_ref,
    energy_ref,
    obs_ref,
    innov_ref,
    valid_ref,
    type_ref,
    inverse_ref,
    out_ref,
    tot_ref,
    anom,
    now,
    prior,
    energy,
    obs,
    innov,
    valid,
    types,
    inverse,
    folded,
    scal,
    mz,
    my,
    mx,
    mz_src,
    my_src,
    mx_src,
    near,
    far_up,
    far_down,
    resp_src,
    resp_in,
    pt_src,
    pt_in,
    load_sem,
    mz_send,
    mz_recv,
    my_send,
    my_recv,
    mx_send,
    mx_recv,
    ob_send,
    ob_recv,
    rs_send,
    rs_recv,
    pt_send,
    pt_recv,
):
    nx, ny, nc, nz = dims
    variables, total_members, lat_rows = counts
    members, slots, rows = obs.shape
    owners = nz // 2
    block = slots // owners
    half = block // 2
    targets = variables * REGIONS
    pair = targets // nz
    lon_tiles = now.shape[1]
    xi = lax.axis_index("lat_0")
    yi = lax.axis_index("lat_1")
    ci = lax.axis_index("lat_2")
    zi = lax.axis_index("lev")

    def loads(pairs, first):
        copies = []
        for i, (a, b) in enumerate(pairs):
            copy = pltpu.make_async_copy(a, b, load_sem.at[first + i])
            copy.start()
            copies.append(copy)
        return copies

    grad_loads = loads([(now_ref, now), (prior_ref, prior), (energy_ref, energy)], 0)
    anom_loads = loads([(anom_ref.at[v], anom.at[v]) for v in range(variables)], 3)

    def z_peer(d):
        return {"lev": lax.rem(zi + d, nz)}

    def x_peer(d):
        return {"lat_0": lax.rem(xi + d, nx)}

    def y_peer(d, e):
        return {"lat_1": lax.rem(yi + d, ny), "lat_2": lax.rem(ci + e, nc)}

    def send(source, target, sems, d, peer):
        copy = pltpu.make_async_remote_copy(
            src_ref=source,
            dst_ref=target,
            send_sem=sems[0].at[d],
            recv_sem=sems[1].at[d],
            device_id=peer,
            device_id_type=MESH,
        )
        copy.start()
        return copy

    def iota(shape, axis):
        return lax.broadcasted_iota(jnp.int32, shape, axis)

    y_steps = [(d, e) for d in ring_order(ny) + [0] for e in range(nc) if d or e]
    barrier = pltpu.get_barrier_semaphore()
    peers = [z_peer(d) for d in ring_order(nz)]
    peers += [y_peer(d, e) for d, e in y_steps]
    peers += [x_peer(d) for d in ring_order(nx)]
    for peer in peers:
        pl.semaphore_signal(barrier, inc=1, device_id=peer, device_id_type=MESH)
    other_loads = loads(
        [
            (obs_ref, obs),
            (innov_ref, innov),
            (valid_ref, valid),
            (type_ref, types),
            (inverse_ref, inverse),
        ],
        3 + variables,
    )

    lat_index = ((xi * ny + yi) * nc + ci) * lat_rows + lax.rem(
        iota((lon_tiles, 128), 0), lat_rows
    )
    cosine = jnp.cos(
        -0.5 * math.pi + ((lat_index + LAT0).astype(F32) + 0.5) * math.pi / NLAT_GRID
    )
    for copy in grad_loads:
        copy.wait()
    spare = jnp.zeros((128 - total_members, 384), BF16)
    for v in range(variables):
        grad = energy[0:1, v : v + 1] * cosine * (now[v] + prior[v])
        grad = grad.astype(BF16).astype(F32)
        anom_loads[v].wait()
        step = 4
        for k in range(0, anom.shape[1], step):
            a = anom[v, k : k + step].astype(F32)
            a = a.reshape(-1, lon_tiles, 128) * grad[None]
            a = a.reshape(a.shape[0], lon_tiles // 8, 8, 128).sum(axis=1)
            folded[v, k * 16 : (k + step) * 16, :] = a.reshape(-1, 128)
    lines = []
    for v in range(variables):
        s = folded[v, pl.ds(0, total_members, stride=8), :]
        for r in range(1, 8):
            s = s + folded[v, pl.ds(r, total_members, stride=8), :]
        high = s.astype(BF16)
        rest = s - high.astype(F32)
        mid = rest.astype(BF16)
        low = (rest - mid.astype(F32)).astype(BF16)
        lines.append(
            jnp.concatenate([jnp.concatenate([high, mid, low], axis=1), spare], axis=0)
        )
    lanes_sum = lax.dot_general(
        jnp.ones((8, 384), BF16),
        jnp.concatenate(lines, axis=0),
        (((1,), (1,)), ((), ())),
        preferred_element_type=F32,
    )
    row4 = iota((4, 128), 0)
    lane4 = iota((4, 128), 1)
    base = jnp.zeros((4, 128), F32)
    for v in range(variables):
        base = jnp.where(row4 == v, lanes_sum[0:4, v * 128 : (v + 1) * 128], base)
    mz_src[0] = base
    mz[pl.ds(zi, 1)] = base[None]

    pl.semaphore_wait(barrier, len(peers))
    z_copies = [
        send(mz_src.at[0], mz.at[zi], (mz_send, mz_recv), d, z_peer(d))
        for d in ring_order(nz)
    ]

    for copy in other_loads:
        copy.wait()
    eye = iota((slots, slots), 0) == iota((slots, slots), 1)

    def column(line):
        wide = jnp.broadcast_to(line.astype(F32), (slots, slots))
        return jnp.sum(jnp.where(eye, wide, 0.0), axis=1, keepdims=True)

    type_col = column(types[...])
    valid_col = column(valid[...])
    inverse_col = jnp.zeros((slots, 1), F32)
    for c in range(NTYPES):
        inverse_col = jnp.where(type_col == c, inverse[0:1, c : c + 1], inverse_col)
    inside = iota((slots, rows), 1).astype(F32) < valid_col
    scaled = innov[...] * inverse_col * inside.astype(F32) / member_scale
    scal[...] = scaled
    onehot = (iota((NTYPES, slots), 0) == types[...]).astype(F32)
    g_add = jnp.zeros((4, 128), F32)
    for m in range(members):
        prod = obs[m].astype(F32) * scal[...]
        by_type = jnp.dot(
            onehot, prod, precision=lax.Precision.HIGHEST, preferred_element_type=F32
        )
        g = jnp.sum(by_type, axis=1, keepdims=True)
        g_add = jnp.where(lane4 == total_members + m, g[0:4], g_add)
        g_add = jnp.where(lane4 == total_members + members + m, g[4:8], g_add)
    my_class = lax.rem(zi, owners)
    mine = pl.ds(pl.multiple_of(my_class * block, block), block)
    near[1] = obs[:, mine, :]

    def select(cols, first):
        wanted = lax.rem(
            zi * members + (first * members + 2 * total_members) + iota((128, cols), 1) // half,
            total_members,
        )
        return (iota((128, cols), 0) == wanted).astype(BF16)

    one = members * half
    sel_near = select(3 * one, -1)
    sel_up = select(one, 2)
    sel_down = select(one, -2)
    row_t = iota((targets * half, targets), 0) // half
    spread = (
        iota((targets * half, targets), 1)
        == lax.rem(row_t, REGIONS) * variables + row_t // REGIONS
    ).astype(BF16)
    sel_own = (
        (iota((128, 128), 0) == iota((128, 128), 1) + zi * members)
        & (iota((128, 128), 1) < members)
    ).astype(BF16)
    perm_r = iota((targets, targets), 0)
    perm = (
        iota((targets, targets), 1) == lax.rem(perm_r, REGIONS) * variables + perm_r // REGIONS
    ).astype(BF16)

    for copy in z_copies:
        copy.wait()
    tot_z = mz[0]
    for z in range(1, nz):
        tot_z = tot_z + mz[z]
    tot_z = tot_z + g_add
    my_src[0] = tot_z
    here_y = yi * nc + ci
    my[pl.ds(here_y, 1)] = tot_z[None]
    y_copies = [
        send(my_src.at[0], my.at[here_y], (my_send, my_recv), d * nc + e, y_peer(d, e))
        for d, e in y_steps
    ]

    def class_at(d, first, size):
        c = lax.rem(zi + d, owners)
        return pl.ds(pl.multiple_of(c * block + first, half), size)

    sems = (ob_send, ob_recv)
    ob_copies = [
        send(obs.at[:, class_at(2, half, half), :], far_down, sems, 0, z_peer(2)),
        send(obs.at[:, class_at(nz - 2, 0, half), :], far_up, sems, 1, z_peer(nz - 2)),
        send(obs.at[:, class_at(1, 0, block), :], near.at[0], sems, 2, z_peer(1)),
        send(obs.at[:, class_at(nz - 1, 0, block), :], near.at[2], sems, 3, z_peer(nz - 1)),
    ]

    for copy in y_copies:
        copy.wait()
    tot_y = my[0]
    for y in range(1, ny * nc):
        tot_y = tot_y + my[y]
    mx_src[0] = tot_y
    mx[pl.ds(xi, 1)] = tot_y[None]
    x_copies = [
        send(mx_src.at[0], mx.at[xi], (mx_send, mx_recv), d, x_peer(d))
        for d in ring_order(nx)
    ]
    for copy in x_copies:
        copy.wait()

    sums = jnp.concatenate([mx[x] for x in range(nx)], axis=0)
    lane16 = iota((targets, 128), 1)
    w = jnp.where(lane16 < total_members, sums / norm_scale, 0.0).astype(BF16)
    g_all = mx[0]
    for x in range(1, nx):
        g_all = g_all + mx[x]

    def diagonal(sel):
        wide = jnp.dot(w, sel, preferred_element_type=F32).astype(BF16)
        tall = jnp.dot(spread, wide, preferred_element_type=F32)
        keep = lax.rem(iota(tall.shape, 0), half) == lax.rem(iota(tall.shape, 1), half)
        return jnp.where(keep, tall, 0.0).astype(BF16)

    wd_near = diagonal(sel_near)
    wd_up = diagonal(sel_up)
    wd_down = diagonal(sel_down)

    w_own = jnp.dot(w, sel_own, preferred_element_type=F32).astype(BF16)
    w_own = jnp.dot(perm, w_own, preferred_element_type=F32)
    g_rows = jnp.concatenate(
        [
            pltpu.roll(g_all, 128 - total_members, 1),
            pltpu.roll(g_all, 128 - total_members - members, 1),
        ],
        axis=0,
    )
    g_rows = jnp.where(iota((NTYPES, 128), 1) < members, g_rows, 0.0)
    share = jnp.zeros((targets, 128), F32)
    for c in range(NTYPES):
        col = jnp.sum(w_own * g_rows[c : c + 1], axis=1, keepdims=True)
        share = jnp.where(lane16 == c, col, share)
    for z in range(nz):
        pt_src[z, 0:pair, :] = share[pair * z : pair * z + pair]
    top = pl.ds(0, pair)
    pt_copies = [
        send(
            pt_src.at[lax.rem(zi + d, nz), top],
            pt_in.at[zi, top],
            (pt_send, pt_recv),
            d,
            z_peer(d),
        )
        for d in ring_order(nz)
    ]
    pt_in[pl.ds(zi, 1), 0:pair, :] = pt_src[pl.ds(zi, 1), 0:pair, :]

    for copy in ob_copies:
        copy.wait()
    rs_copies = []
    for g, (wd_far, far) in enumerate(((wd_up, far_up), (wd_down, far_down))):
        part = pl.ds(g * half, half)
        close = near[:, :, g * half : (g + 1) * half, :].reshape(3 * one, rows)
        answered = jnp.dot(wd_near, close, preferred_element_type=F32)
        answered += jnp.dot(
            wd_far, far[...].reshape(one, rows), preferred_element_type=F32
        )
        resp_src[:, g] = answered.astype(BF16).reshape(nz, pair, half, rows)
        for d in ring_order(nz):
            rs_copies.append(
                send(
                    resp_src.at[lax.rem(zi + d, nz), g],
                    resp_in.at[zi, g],
                    (rs_send, rs_recv),
                    g * nz + d,
                    z_peer(d),
                )
            )
    resp_in[pl.ds(zi, 1)] = resp_src[pl.ds(zi, 1)]

    for copy in rs_copies:
        copy.wait()
    for c in range(owners):
        for g in range(2):
            first = c * block + g * half
            for t in range(pair):
                value = resp_in[c, g, t].astype(F32) + resp_in[c + owners, g, t].astype(F32)
                value = value * scal[first : first + half, :]
                for lane in range(rows // 128):
                    place = (first * (rows // 128) + lane) * pair + t
                    out_ref[pl.ds(place, half, stride=pair * (rows // 128)), :] = value[
                        :, lane * 128 : (lane + 1) * 128
                    ]
    for copy in pt_copies:
        copy.wait()
    whole = pt_in[0, 0:pair, :]
    for z in range(1, nz):
        whole = whole + pt_in[z, 0:pair, :]
    tot_ref[...] = whole[:, 0:NTYPES] / total_scale


def local(
    anomalies,
    error_now,
    error_prior,
    energy_coef,
    obs_anomalies,
    innovations,
    valid_counts,
    type_ids,
    error_inverse,
):
    dims = tuple(lax.axis_size(a) for a in (*LAT, "lev"))
    nx, ny, nc, nz = dims
    variables, levels, members, lat_rows, lon_count = anomalies.shape
    slots, local_members, rows = obs_anomalies.shape
    lat_total = lat_rows * nx * ny * nc
    norm_scale = math.sqrt(levels * nz * lat_total * lon_count / REGIONS)
    member_scale = math.sqrt(members - 1)
    total_scale = math.sqrt(slots * nx * ny * nc * rows / NTYPES)
    targets = variables * REGIONS
    pair = targets // nz
    block = slots // (nz // 2)
    half = block // 2
    tiles = lon_count // 128 * lat_rows

    def by_tile(a):
        a = a.reshape(*a.shape[:-1], lon_count // 128, 128)
        n = a.ndim
        order = (*range(n - 3), n - 2, n - 3, n - 1)
        a = with_layout_constraint(a, Layout(major_to_minor=order))
        a = jnp.swapaxes(a, -3, -2)
        return a.reshape(*a.shape[:-3], tiles, 128)

    anom = by_tile(anomalies[:, 0]).reshape(variables, members // 2, 2 * tiles, 128)
    now = by_tile(error_now[:, 0])
    prior = by_tile(error_prior[:, 0])
    obs = jnp.transpose(obs_anomalies, (1, 0, 2))
    inputs = (
        anom,
        now,
        prior,
        energy_coef.reshape(1, variables),
        obs,
        innovations,
        valid_counts.reshape(1, slots),
        type_ids.reshape(1, slots),
        error_inverse.reshape(1, NTYPES),
    )
    vmem = pl.BlockSpec(memory_space=pltpu.VMEM)
    hbm = pl.BlockSpec(memory_space=pltpu.HBM)
    dma = pltpu.SemaphoreType.DMA
    table = pltpu.VMEM
    out, totals = pl.pallas_call(
        functools.partial(
            exchange_kernel,
            dims,
            (variables, members, lat_rows),
            norm_scale,
            member_scale,
            total_scale,
        ),
        out_shape=(
            jax.ShapeDtypeStruct((slots * pair * rows // 128, 128), F32),
            jax.ShapeDtypeStruct((pair, NTYPES), F32),
        ),
        in_specs=[hbm] * len(inputs),
        out_specs=(vmem, vmem),
        scratch_shapes=[table(a.shape, a.dtype) for a in inputs]
        + [
            table((variables, members * 8, 128), F32),
            table((slots, rows), F32),
            table((nz, 4, 128), F32),
            table((ny * nc, 4, 128), F32),
            table((nx, 4, 128), F32),
            table((1, 4, 128), F32),
            table((1, 4, 128), F32),
            table((1, 4, 128), F32),
            table((3, local_members, block, rows), BF16),
            table((local_members, half, rows), BF16),
            table((local_members, half, rows), BF16),
            table((nz, 2, pair, half, rows), BF16),
            table((nz, 2, pair, half, rows), BF16),
            table((nz, 8, 128), F32),
            table((nz, 8, 128), F32),
            dma((8 + variables,)),
            dma((nz,)),
            dma((nz,)),
            dma((ny * nc,)),
            dma((ny * nc,)),
            dma((nx,)),
            dma((nx,)),
            dma((4,)),
            dma((4,)),
            dma((2 * nz,)),
            dma((2 * nz,)),
            dma((nz,)),
            dma((nz,)),
        ],
        compiler_params=pltpu.CompilerParams(
            collective_id=0, has_side_effects=True, vmem_limit_bytes=24 * 1024 * 1024
        ),
    )(*(pltpu.with_memory_space_constraint(a, pltpu.HBM) for a in inputs))
    impact = out.reshape(slots, rows // 128, pair, 128)
    impact = jnp.transpose(impact, (0, 2, 1, 3)).reshape(slots, pair, rows)
    return (impact, totals)


def solution(mesh):
    split = Mesh(
        mesh.devices.reshape(4, 8, 2, mesh.shape["lev"]), ("lat_0", "lat_1", "lat_2", "lev")
    )
    in_specs = (
        P(None, "lev", None, LAT, None),
        P(None, "lev", LAT, None),
        P(None, "lev", LAT, None),
        P(None, "lev"),
        P(LAT, "lev", None),
        P(LAT, None),
        P(LAT),
        P(LAT),
        P(),
    )
    out_specs = (P(LAT, "lev", None), P("lev", None))
    return jax.shard_map(local, mesh=split, in_specs=in_specs, out_specs=out_specs, check_vma=False)
```

```python
import functools
import math

import jax
import jax.numpy as jnp
from jax import lax
from jax.experimental.layout import Layout, with_layout_constraint
from jax.experimental import pallas as pl
from jax.experimental.pallas import tpu as pltpu
from jax.sharding import Mesh
from jax.sharding import PartitionSpec as P

NLAT_GRID = 768
LAT0 = 256
REGIONS = 4
NTYPES = 8
LAT = ("lat_0", "lat_1", "lat_2")
MESH = pl.DeviceIdType.MESH
EARLY = True
SHARES = (1, 1, 1)
F32 = jnp.float32
BF16 = jnp.bfloat16


def ring_order(n):
    return sorted(range(1, n), key=lambda d: (-min(d, n - d), d))


def exchange_kernel(
    dims,
    counts,
    shares,
    norm_scale,
    member_scale,
    total_scale,
    anom_ref,
    now_ref,
    prior_ref,
    energy_ref,
    obs_ref,
    innov_ref,
    valid_ref,
    type_ref,
    inverse_ref,
    out_ref,
    tot_ref,
    anom,
    errors,
    energy,
    obs,
    innov,
    valid,
    types,
    inverse,
    folded,
    scal,
    mz,
    my,
    mx,
    sums_src,
    g_in,
    near,
    far_up,
    far_down,
    single,
    packed,
    packed_single,
    resp_src,
    resp_in,
    pt_src,
    pt_in,
    load_sem,
    mz_sem,
    g_sem,
    my_sem,
    mx_sem,
    ob_sem,
    rs_sem,
    pt_sem,
):
    nx, ny, nc, nz = dims
    variables, total_members, lat_rows = counts
    n_up, n_down, n_single = shares
    groups, members, eight, rows = obs.shape
    slots = groups * eight
    owners = nz // 2
    double = n_up + n_down
    single_base = owners * double
    pieces = double + n_single
    targets = variables * REGIONS
    pair = targets // nz
    lon_tiles = errors.shape[2]
    one = members * eight
    xi = lax.axis_index("lat_0")
    yi = lax.axis_index("lat_1")
    ci = lax.axis_index("lat_2")
    zi = lax.axis_index("lev")
    lead = nc - 1

    def z_peer(d, core=None):
        peer = {"lev": lax.rem(zi + d, nz)}
        if core is not None:
            peer["lat_2"] = core
        return peer

    def x_peer(d, core=None):
        peer = {"lat_0": lax.rem(xi + d, nx)}
        if core is not None:
            peer["lat_2"] = core
        return peer

    def y_peer(d):
        return {"lat_1": lax.rem(yi + d, ny)}

    def remote(source, target, send_sem, recv_sem, peer):
        return pltpu.make_async_remote_copy(
            src_ref=source,
            dst_ref=target,
            send_sem=send_sem,
            recv_sem=recv_sem,
            device_id=peer,
            device_id_type=MESH,
        )

    def send(source, target, send_sem, recv_sem, peer):
        remote(source, target, send_sem, recv_sem, peer).start()

    def iota(shape, axis):
        return lax.broadcasted_iota(jnp.int32, shape, axis)

    barrier = pltpu.get_barrier_semaphore()
    other_core = nc - 1 - ci
    partner = {"lat_2": other_core}

    def greet(hops):
        for _, peer in sorted(hops, key=lambda h: -h[0]):
            pl.semaphore_signal(barrier, inc=1, device_id=peer, device_id_type=MESH)

    def far(d, n):
        return min(d, n - d)

    z_same = [(far(d, nz), z_peer(d)) for d in ring_order(nz)]
    x_lead = [(far(d, nx), x_peer(d, lead)) for d in ring_order(nx)]

    @pl.when(ci == lead)
    def _():
        z_other = [(far(d, nz), z_peer(d, other_core)) for d in ring_order(nz)]
        along_y = [(far(d, ny), y_peer(d)) for d in ring_order(ny)]
        greet(z_same + z_other + along_y + x_lead + [(0, partner)])

    @pl.when(ci != lead)
    def _():
        greet(z_same + x_lead + [(0, partner)])

    def load(source, target, n):
        pltpu.make_async_copy(source, target, load_sem.at[n]).start()

    def landed(target, sem):
        pltpu.make_async_copy(target, target, sem).wait()

    load(now_ref, errors.at[0], 0)
    load(prior_ref, errors.at[1], 0)
    load(energy_ref, energy, 1)
    for v in range(variables):
        load(anom_ref.at[v], anom.at[v], 6 + v)
    for m in range(members):
        load(obs_ref.at[m], obs.at[:, m], 6 + variables)
    load(innov_ref, innov, 2)
    load(valid_ref, valid, 3)
    load(type_ref, types, 4)
    load(inverse_ref, inverse, 5)

    lat_index = ((xi * ny + yi) * nc + ci) * lat_rows + lax.rem(
        iota((lon_tiles, 128), 0), lat_rows
    )
    cosine = jnp.cos(
        -0.5 * math.pi + ((lat_index + LAT0).astype(F32) + 0.5) * math.pi / NLAT_GRID
    )
    landed(errors, load_sem.at[0])
    landed(energy, load_sem.at[1])
    spare = jnp.zeros((128 - total_members, 384), BF16)
    for v in range(variables):
        grad = energy[0:1, v : v + 1] * cosine * (errors[0, v] + errors[1, v])
        grad = grad.astype(BF16).astype(F32)
        landed(anom.at[v], load_sem.at[6 + v])
        step = 4
        for k in range(0, anom.shape[1], step):
            a = anom[v, k : k + step].astype(F32)
            a = a.reshape(-1, lon_tiles, 128) * grad[None]
            a = a.reshape(a.shape[0], lon_tiles // 8, 8, 128).sum(axis=1)
            folded[v, k * 16 : (k + step) * 16, :] = a.reshape(-1, 128)
    lines = []
    for v in range(variables):
        s = folded[v, pl.ds(0, total_members, stride=8), :]
        for r in range(1, 8):
            s = s + folded[v, pl.ds(r, total_members, stride=8), :]
        high = s.astype(BF16)
        rest = s - high.astype(F32)
        mid = rest.astype(BF16)
        low = (rest - mid.astype(F32)).astype(BF16)
        lines.append(
            jnp.concatenate([jnp.concatenate([high, mid, low], axis=1), spare], axis=0)
        )
    lanes_sum = lax.dot_general(
        jnp.ones((8, 384), BF16),
        jnp.concatenate(lines, axis=0),
        (((1,), (1,)), ((), ())),
        preferred_element_type=F32,
    )
    row4 = iota((4, 128), 0)
    lane4 = iota((4, 128), 1)
    base = jnp.zeros((4, 128), F32)
    for v in range(variables):
        base = jnp.where(row4 == v, lanes_sum[0:4, v * 128 : (v + 1) * 128], base)
    sums_src[0] = base
    here_z = zi * nc + ci
    mz[pl.ds(here_z, 1)] = base[None]

    def z_copy(d):
        return remote(
            sums_src.at[0],
            mz.at[here_z],
            mz_sem.at[0],
            mz_sem.at[1],
            z_peer(d, lead),
        )

    @pl.when(ci == lead)
    def _():
        pl.semaphore_wait(barrier, nz - 1 + ny - 1 + nc * (nx - 1) + 1)

    @pl.when(ci != lead)
    def _():
        pl.semaphore_wait(barrier, nc * (nz - 1) + 1)

    for d in ring_order(nz):
        z_copy(d).start()

    @pl.when(ci != lead)
    def _():
        z_copy(0).start()

    def obs_copies():
        def double_at(d, first, size):
            c = lax.rem(zi + d, owners)
            return pl.ds(c * double + first, size)

        far = nz - 2
        send(obs.at[double_at(2, n_up, n_down)], far_down, ob_sem.at[0], ob_sem.at[1], z_peer(2))
        send(obs.at[double_at(far, 0, n_up)], far_up, ob_sem.at[2], ob_sem.at[3], z_peer(far))
        if n_single:
            for d in ring_order(nz):
                there = pl.ds(single_base + lax.rem(zi + d, nz) * n_single, n_single)
                send(obs.at[there], single.at[zi], ob_sem.at[6], ob_sem.at[7], z_peer(d))
        for d, slot in ((1, 0), (nz - 1, 2)):
            source = obs.at[double_at(d, 0, double)]
            send(source, near.at[slot], ob_sem.at[4], ob_sem.at[5], z_peer(d))

    landed(obs, load_sem.at[6 + variables])
    if EARLY:
        obs_copies()

    landed(innov, load_sem.at[2])
    landed(valid, load_sem.at[3])
    landed(types, load_sem.at[4])
    landed(inverse, load_sem.at[5])
    eye = iota((slots, slots), 0) == iota((slots, slots), 1)

    def column(line):
        wide = jnp.broadcast_to(line.astype(F32), (slots, slots))
        return jnp.sum(jnp.where(eye, wide, 0.0), axis=1, keepdims=True)

    type_col = column(types[...])
    valid_col = column(valid[...])
    inverse_col = jnp.zeros((slots, 1), F32)
    for c in range(NTYPES):
        inverse_col = jnp.where(type_col == c, inverse[0:1, c : c + 1], inverse_col)
    inside = iota((slots, rows), 1).astype(F32) < valid_col
    scal[...] = innov[...] * inverse_col * inside.astype(F32) / member_scale
    onehot = (iota((NTYPES, slots), 0) == types[...]).astype(BF16)
    onehot = jnp.concatenate([onehot, onehot], axis=1)
    g_add = jnp.zeros((4, 128), F32)
    for m in range(members):
        prod = obs[:, m].astype(F32).reshape(slots, rows) * scal[...]
        high = prod.astype(BF16)
        low = (prod - high.astype(F32)).astype(BF16)
        by_type = jnp.dot(
            onehot, jnp.concatenate([high, low], axis=0), preferred_element_type=F32
        )
        g = jnp.sum(by_type, axis=1, keepdims=True)
        g_add = jnp.where(lane4 == total_members + m, g[0:4], g_add)
        g_add = jnp.where(lane4 == total_members + members + m, g[4:8], g_add)
    sums_src[1] = g_add

    def g_copy():
        return remote(
            sums_src.at[1], g_in.at[0], g_sem.at[0], g_sem.at[1], {"lat_2": other_core}
        )

    @pl.when(ci != lead)
    def _():
        g_copy().start()

    my_class = lax.rem(zi, owners)
    near[1] = obs[pl.ds(my_class * double, double)]
    if n_single:
        single[pl.ds(zi, 1)] = obs[pl.ds(single_base + zi * n_single, n_single)][None]

    width = 4 * one
    pitch = -(-width // 128) * 128
    spot = iota((128, pitch), 1)

    def select(first):
        wanted = lax.rem(
            (zi + nz + first) * members + spot // eight, total_members
        )
        return ((iota((128, pitch), 0) == wanted) & (spot < width)).astype(BF16)

    tables = [select(-1), select(-2)]
    if n_single:
        shape = (128, nz * one)
        tables.append((iota(shape, 0) == iota(shape, 1) // eight).astype(BF16))
    sel = jnp.concatenate(tables, axis=1)
    row_t = iota((targets * eight, targets), 0) // eight
    spread = (
        iota((targets * eight, targets), 1)
        == lax.rem(row_t, REGIONS) * variables + row_t // REGIONS
    ).astype(BF16)
    sel_own = (
        (iota((128, 128), 0) == iota((128, 128), 1) + zi * members)
        & (iota((128, 128), 1) < members)
    ).astype(BF16)
    perm_r = iota((targets, targets), 0)
    perm = (
        iota((targets, targets), 1) == lax.rem(perm_r, REGIONS) * variables + perm_r // REGIONS
    ).astype(BF16)

    def y_copy(d):
        return remote(
            sums_src.at[2], my.at[yi], my_sem.at[0], my_sem.at[1], y_peer(d)
        )

    def x_copy(d, core):
        return remote(
            sums_src.at[3],
            mx.at[xi],
            mx_sem.at[0],
            mx_sem.at[1],
            x_peer(d, core),
        )

    @pl.when(ci == lead)
    def _():
        g_copy().wait_recv()
        landed(mz.at[pl.ds(0, nz * nc - 1)], mz_sem.at[1])
        total = mz[0]
        for z in range(1, nz * nc):
            total = total + mz[z]
        total = total + g_add + g_in[0]
        sums_src[2] = total
        my[pl.ds(yi, 1)] = total[None]
        for d in ring_order(ny):
            y_copy(d).start()

    if not EARLY:
        obs_copies()

    @pl.when(ci == lead)
    def _():
        landed(my.at[pl.ds(0, ny - 1)], my_sem.at[1])
        total = my[0]
        for y in range(1, ny):
            total = total + my[y]
        sums_src[3] = total
        mx[pl.ds(xi, 1)] = total[None]
        for d in ring_order(nx) + [0]:
            for core in range(nc):
                if d or core != lead:
                    x_copy(d, core).start()

    landed(far_down, ob_sem.at[1])
    landed(far_up, ob_sem.at[3])
    landed(near.at[pl.ds(0, 2)], ob_sem.at[5])
    if n_single:
        landed(single.at[pl.ds(0, nz - 1)], ob_sem.at[7])

    def rows_of(value):
        return value.astype(F32).reshape(-1, rows).astype(BF16)

    for p in range(double):
        close = rows_of(near[:, p])
        if p < n_up:
            packed[p, 0 : 3 * one, :] = close
            packed[p, 3 * one : width, :] = rows_of(far_up[p])
        else:
            packed[p, one:width, :] = close
            packed[p, 0:one, :] = rows_of(far_down[p - n_up])
    for p in range(n_single):
        packed_single[p] = rows_of(single[:, p])

    @pl.when(ci == lead)
    def _():
        landed(mx.at[pl.ds(0, nx - 1)], mx_sem.at[1])

    @pl.when(ci != lead)
    def _():
        landed(mx, mx_sem.at[1])

    sums = jnp.concatenate([mx[x] for x in range(nx)], axis=0)
    lane16 = iota((targets, 128), 1)
    w = jnp.where(lane16 < total_members, sums / norm_scale, 0.0).astype(BF16)
    wide = jnp.dot(w, sel, preferred_element_type=F32).astype(BF16)
    tall = jnp.dot(spread, wide, preferred_element_type=F32)
    keep = lax.rem(iota(tall.shape, 0), eight) == lax.rem(iota(tall.shape, 1), eight)
    wd = jnp.where(keep, tall, 0.0).astype(BF16)

    for p in range(pieces):
        if p < double:
            first = 0 if p < n_up else pitch
            answered = jnp.dot(
                wd[:, first : first + width], packed[p], preferred_element_type=F32
            )
        else:
            answered = jnp.dot(
                wd[:, 2 * pitch :], packed_single[p - double], preferred_element_type=F32
            )
        resp_src[:, p] = answered.astype(BF16).reshape(nz, pair * eight, rows)
        for d in ring_order(nz):
            send(
                resp_src.at[lax.rem(zi + d, nz), p],
                resp_in.at[zi, p],
                rs_sem.at[pieces],
                rs_sem.at[p],
                z_peer(d),
            )

    g_all = mx[0]
    for x in range(1, nx):
        g_all = g_all + mx[x]
    w_own = jnp.dot(w, sel_own, preferred_element_type=F32).astype(BF16)
    w_own = jnp.dot(perm, w_own, preferred_element_type=F32)
    g_rows = jnp.concatenate(
        [
            pltpu.roll(g_all, 128 - total_members, 1),
            pltpu.roll(g_all, 128 - total_members - members, 1),
        ],
        axis=0,
    )
    g_rows = jnp.where(iota((NTYPES, 128), 1) < members, g_rows, 0.0)
    share = jnp.zeros((targets, 128), F32)
    for c in range(NTYPES):
        col = jnp.sum(w_own * g_rows[c : c + 1], axis=1, keepdims=True)
        share = jnp.where(lane16 == c, col, share)
    for z in range(nz):
        pt_src[z, 0:pair, :] = share[pair * z : pair * z + pair]
    top = pl.ds(0, pair)
    for d in ring_order(nz):
        other = lax.rem(zi + d, nz)
        send(pt_src.at[other, top], pt_in.at[zi, top], pt_sem.at[0], pt_sem.at[1], z_peer(d))
    pt_in[pl.ds(zi, 1), 0:pair, :] = pt_src[pl.ds(zi, 1), 0:pair, :]
    resp_in[pl.ds(zi, 1)] = resp_src[pl.ds(zi, 1)]

    def place(value, group):
        start = group * eight
        for t in range(pair):
            line = value[t * eight : (t + 1) * eight] * scal[start : start + eight, :]
            for lane in range(rows // 128):
                spot = (start * (rows // 128) + lane) * pair + t
                out_ref[pl.ds(spot, eight, stride=pair * (rows // 128)), :] = line[
                    :, lane * 128 : (lane + 1) * 128
                ]

    for p in range(pieces):
        landed(resp_in.at[pl.ds(0, nz - 1), p], rs_sem.at[p])
        if p < double:
            for c in range(owners):
                value = resp_in[c, p].astype(F32) + resp_in[c + owners, p].astype(F32)
                place(value, c * double + p)
        else:
            for z in range(nz):
                place(resp_in[z, p].astype(F32), single_base + z * n_single + p - double)
    landed(pt_in.at[pl.ds(0, nz - 1), top], pt_sem.at[1])
    whole = pt_in[0, 0:pair, :]
    for z in range(1, nz):
        whole = whole + pt_in[z, 0:pair, :]
    tot_ref[...] = whole[:, 0:NTYPES] / total_scale

    landed(far_down, ob_sem.at[0])
    landed(far_up, ob_sem.at[2])
    landed(near.at[pl.ds(0, 2)], ob_sem.at[4])
    if n_single:
        landed(single.at[pl.ds(0, nz - 1)], ob_sem.at[6])
    landed(resp_src.at[pl.ds(0, nz - 1)], rs_sem.at[pieces])
    landed(pt_src.at[pl.ds(0, nz - 1), top], pt_sem.at[0])

    @pl.when(ci != lead)
    def _():
        landed(mz.at[pl.ds(0, nz)], mz_sem.at[0])
        g_copy().wait_send()

    @pl.when(ci == lead)
    def _():
        landed(mz.at[pl.ds(0, nz - 1)], mz_sem.at[0])
        landed(my.at[pl.ds(0, ny - 1)], my_sem.at[0])
        landed(mz.at[pl.ds(0, nx * nc - 1)], mx_sem.at[0])


def store_kernel(out_ref, tot_ref, out_hbm, tot_hbm, sems):
    copies = [
        pltpu.make_async_copy(out_ref, out_hbm, sems.at[0]),
        pltpu.make_async_copy(tot_ref, tot_hbm, sems.at[1]),
    ]
    for copy in copies:
        copy.start()
    for copy in copies:
        copy.wait()


def local(
    anomalies,
    error_now,
    error_prior,
    energy_coef,
    obs_anomalies,
    innovations,
    valid_counts,
    type_ids,
    error_inverse,
):
    dims = tuple(lax.axis_size(a) for a in (*LAT, "lev"))
    nx, ny, nc, nz = dims
    variables, levels, members, lat_rows, lon_count = anomalies.shape
    slots, local_members, rows = obs_anomalies.shape
    lat_total = lat_rows * nx * ny * nc
    norm_scale = math.sqrt(levels * nz * lat_total * lon_count / REGIONS)
    member_scale = math.sqrt(members - 1)
    total_scale = math.sqrt(slots * nx * ny * nc * rows / NTYPES)
    targets = variables * REGIONS
    pair = targets // nz
    n_up, n_down, n_single = SHARES
    double = n_up + n_down
    pieces = double + n_single
    tiles = lon_count // 128 * lat_rows

    def by_tile(a):
        a = a.reshape(*a.shape[:-1], lon_count // 128, 128)
        n = a.ndim
        order = (*range(n - 3), n - 2, n - 3, n - 1)
        a = with_layout_constraint(a, Layout(major_to_minor=order))
        a = jnp.swapaxes(a, -3, -2)
        return a.reshape(*a.shape[:-3], tiles, 128)

    anom = by_tile(anomalies[:, 0]).reshape(variables, members // 2, 2 * tiles, 128)
    now = by_tile(error_now[:, 0])
    prior = by_tile(error_prior[:, 0])
    obs = jnp.transpose(obs_anomalies, (1, 0, 2)).reshape(local_members, slots // 8, 8, rows)
    inputs = (
        anom,
        now,
        prior,
        energy_coef.reshape(1, variables),
        obs,
        innovations,
        valid_counts.reshape(1, slots),
        type_ids.reshape(1, slots),
        error_inverse.reshape(1, NTYPES),
    )
    vmem = pl.BlockSpec(memory_space=pltpu.VMEM)
    hbm = pl.BlockSpec(memory_space=pltpu.HBM)
    dma = pltpu.SemaphoreType.DMA
    table = pltpu.VMEM
    out, totals = pl.pallas_call(
        functools.partial(
            exchange_kernel,
            dims,
            (variables, members, lat_rows),
            SHARES,
            norm_scale,
            member_scale,
            total_scale,
        ),
        out_shape=(
            jax.ShapeDtypeStruct((slots * pair * rows // 128, 128), F32),
            jax.ShapeDtypeStruct((pair, NTYPES), F32),
        ),
        in_specs=[hbm] * len(inputs),
        out_specs=(vmem, vmem),
        scratch_shapes=[
            table(anom.shape, BF16),
            table((2, *now.shape), F32),
            table((1, variables), F32),
            table((slots // 8, local_members, 8, rows), BF16),
            table((slots, rows), F32),
            table((1, slots), jnp.int32),
            table((1, slots), jnp.int32),
            table((1, NTYPES), F32),
        ]
        + [
            table((variables, members * 8, 128), F32),
            table((slots, rows), F32),
            table((nz * nc, 4, 128), F32),
            table((ny, 4, 128), F32),
            table((nx, 4, 128), F32),
            table((4, 4, 128), F32),
            table((1, 4, 128), F32),
            table((3, double, local_members, 8, rows), BF16),
            table((n_up, local_members, 8, rows), BF16),
            table((n_down, local_members, 8, rows), BF16),
            table((nz, max(n_single, 1), local_members, 8, rows), BF16),
            table((double, 32 * local_members, rows), BF16),
            table((max(n_single, 1), 8 * nz * local_members, rows), BF16),
            table((nz, pieces, pair * 8, rows), BF16),
            table((nz, pieces, pair * 8, rows), BF16),
            table((nz, 8, 128), F32),
            table((nz, 8, 128), F32),
            dma((7 + variables,)),
            dma((2,)),
            dma((2,)),
            dma((2,)),
            dma((2,)),
            dma((8,)),
            dma((pieces + 1,)),
            dma((2,)),
        ],
        compiler_params=pltpu.CompilerParams(
            collective_id=0, has_side_effects=True, vmem_limit_bytes=24 * 1024 * 1024
        ),
    )(*(pltpu.with_memory_space_constraint(a, pltpu.HBM) for a in inputs))
    out, totals = pl.pallas_call(
        store_kernel,
        out_shape=(pltpu.HBM(out.shape, F32), pltpu.HBM(totals.shape, F32)),
        in_specs=[vmem, vmem],
        out_specs=(hbm, hbm),
        scratch_shapes=[dma((2,))],
        compiler_params=pltpu.CompilerParams(vmem_limit_bytes=4 * 1024 * 1024),
    )(out, totals)
    impact = out.reshape(slots, rows // 128, pair, 128)
    impact = jnp.transpose(impact, (0, 2, 1, 3)).reshape(slots, pair, rows)
    return (impact, totals)


def solution(mesh):
    split = Mesh(
        mesh.devices.reshape(4, 8, 2, mesh.shape["lev"]), ("lat_0", "lat_1", "lat_2", "lev")
    )
    in_specs = (
        P(None, "lev", None, LAT, None),
        P(None, "lev", LAT, None),
        P(None, "lev", LAT, None),
        P(None, "lev"),
        P(LAT, "lev", None),
        P(LAT, None),
        P(LAT),
        P(LAT),
        P(),
    )
    out_specs = (P(LAT, "lev", None), P("lev", None))
    return jax.shard_map(local, mesh=split, in_specs=in_specs, out_specs=out_specs, check_vma=False)
```

```python
import functools
import math

import jax
import jax.numpy as jnp
from jax import lax
from jax.experimental.layout import Layout, with_layout_constraint
from jax.experimental import pallas as pl
from jax.experimental.pallas import tpu as pltpu
from jax.sharding import Mesh
from jax.sharding import PartitionSpec as P

NLAT_GRID = 768
LAT0 = 256
REGIONS = 4
NTYPES = 8
LAT = ("lat_0", "lat_1", "lat_2")
MESH = pl.DeviceIdType.MESH
EARLY = True
SHARES = (2, 0, 1)
F32 = jnp.float32
BF16 = jnp.bfloat16


def ring_order(n):
    return sorted(range(1, n), key=lambda d: (-min(d, n - d), d))


def exchange_kernel(
    dims,
    counts,
    shares,
    norm_scale,
    member_scale,
    total_scale,
    anom_ref,
    now_ref,
    prior_ref,
    energy_ref,
    obs_ref,
    innov_ref,
    valid_ref,
    type_ref,
    inverse_ref,
    out_ref,
    tot_ref,
    anom,
    errors,
    energy,
    obs,
    innov,
    valid,
    types,
    inverse,
    folded,
    scal,
    mz,
    my,
    mx,
    sums_src,
    g_in,
    near,
    far_up,
    far_down,
    single,
    packed,
    packed_single,
    resp_src,
    resp_in,
    pt_src,
    pt_in,
    load_sem,
    mz_sem,
    g_sem,
    my_sem,
    mx_sem,
    ob_sem,
    rs_sem,
    pt_sem,
):
    nx, ny, nc, nz = dims
    variables, total_members, lat_rows = counts
    n_up, n_down, n_single = shares
    groups, members, eight, rows = obs.shape
    slots = groups * eight
    owners = nz // 2
    double = n_up + n_down
    single_base = owners * double
    pieces = double + n_single
    targets = variables * REGIONS
    pair = targets // nz
    lon_tiles = errors.shape[2]
    one = members * eight
    xi = lax.axis_index("lat_0")
    yi = lax.axis_index("lat_1")
    ci = lax.axis_index("lat_2")
    zi = lax.axis_index("lev")
    lead = nc - 1

    def z_peer(d, core=None):
        peer = {"lev": lax.rem(zi + d, nz)}
        if core is not None:
            peer["lat_2"] = core
        return peer

    def x_peer(d, core=None):
        peer = {"lat_0": lax.rem(xi + d, nx)}
        if core is not None:
            peer["lat_2"] = core
        return peer

    def y_peer(d):
        return {"lat_1": lax.rem(yi + d, ny)}

    def remote(source, target, send_sem, recv_sem, peer):
        return pltpu.make_async_remote_copy(
            src_ref=source,
            dst_ref=target,
            send_sem=send_sem,
            recv_sem=recv_sem,
            device_id=peer,
            device_id_type=MESH,
        )

    def send(source, target, send_sem, recv_sem, peer):
        remote(source, target, send_sem, recv_sem, peer).start()

    def iota(shape, axis):
        return lax.broadcasted_iota(jnp.int32, shape, axis)

    barrier = pltpu.get_barrier_semaphore()
    other_core = nc - 1 - ci
    partner = {"lat_2": other_core}

    def greet(hops):
        for _, peer in sorted(hops, key=lambda h: -h[0]):
            pl.semaphore_signal(barrier, inc=1, device_id=peer, device_id_type=MESH)

    def far(d, n):
        return min(d, n - d)

    z_same = [(far(d, nz), z_peer(d)) for d in ring_order(nz)]
    x_lead = [(far(d, nx), x_peer(d, lead)) for d in ring_order(nx)]

    @pl.when(ci == lead)
    def _():
        z_other = [(far(d, nz), z_peer(d, other_core)) for d in ring_order(nz)]
        along_y = [(far(d, ny), y_peer(d)) for d in ring_order(ny)]
        greet(z_same + z_other + along_y + x_lead + [(0, partner)])

    @pl.when(ci != lead)
    def _():
        greet(z_same + x_lead + [(0, partner)])

    def load(source, target, n):
        pltpu.make_async_copy(source, target, load_sem.at[n]).start()

    def landed(target, sem):
        pltpu.make_async_copy(target, target, sem).wait()

    load(now_ref, errors.at[0], 0)
    load(prior_ref, errors.at[1], 0)
    load(energy_ref, energy, 1)
    for v in range(variables):
        load(anom_ref.at[v], anom.at[v], 6 + v)
    for m in range(members):
        load(obs_ref.at[m], obs.at[:, m], 6 + variables)
    load(innov_ref, innov, 2)
    load(valid_ref, valid, 3)
    load(type_ref, types, 4)
    load(inverse_ref, inverse, 5)

    lat_index = ((xi * ny + yi) * nc + ci) * lat_rows + lax.rem(
        iota((lon_tiles, 128), 0), lat_rows
    )
    cosine = jnp.cos(
        -0.5 * math.pi + ((lat_index + LAT0).astype(F32) + 0.5) * math.pi / NLAT_GRID
    )
    landed(errors, load_sem.at[0])
    landed(energy, load_sem.at[1])
    for v in range(variables):
        grad = energy[0:1, v : v + 1] * cosine * (errors[0, v] + errors[1, v])
        grad = grad.astype(BF16).astype(F32)
        landed(anom.at[v], load_sem.at[6 + v])
        step = 4
        for k in range(0, anom.shape[1], step):
            a = anom[v, k : k + step].astype(F32)
            a = a.reshape(-1, lon_tiles, 128) * grad[None]
            a = a.reshape(a.shape[0], lon_tiles // 8, 8, 128).sum(axis=1)
            folded[v, k * 16 : (k + step) * 16, :] = a.reshape(-1, 128)
    lane80 = iota((total_members, 128), 1)
    flat = jnp.zeros((total_members, 128), F32)
    for v in range(variables):
        s = folded[v, pl.ds(0, total_members, stride=8), :]
        for r in range(1, 8):
            s = s + folded[v, pl.ds(r, total_members, stride=8), :]
        flat = jnp.where(lane80 == v, jnp.sum(s, axis=1, keepdims=True), flat)
    flat = jnp.concatenate([flat, jnp.zeros((128 - total_members, 128), F32)], axis=0)
    base = jnp.transpose(flat)[0:4]
    lane4 = iota((4, 128), 1)
    sums_src[0] = base
    here_z = zi * nc + ci
    mz[pl.ds(here_z, 1)] = base[None]

    def z_copy(d):
        return remote(
            sums_src.at[0],
            mz.at[here_z],
            mz_sem.at[0],
            mz_sem.at[1],
            z_peer(d, lead),
        )

    @pl.when(ci == lead)
    def _():
        pl.semaphore_wait(barrier, nz - 1 + ny - 1 + nc * (nx - 1) + 1)

    @pl.when(ci != lead)
    def _():
        pl.semaphore_wait(barrier, nc * (nz - 1) + 1)

    for d in ring_order(nz):
        z_copy(d).start()

    @pl.when(ci != lead)
    def _():
        z_copy(0).start()

    def obs_copies():
        def double_at(d, first, size):
            c = lax.rem(zi + d, owners)
            return pl.ds(c * double + first, size)

        far = nz - 2
        if n_down:
            send(obs.at[double_at(2, n_up, n_down)], far_down, ob_sem.at[0], ob_sem.at[1], z_peer(2))
        if n_up:
            send(obs.at[double_at(far, 0, n_up)], far_up, ob_sem.at[2], ob_sem.at[3], z_peer(far))
        if n_single:
            for d in ring_order(nz):
                there = pl.ds(single_base + lax.rem(zi + d, nz) * n_single, n_single)
                send(obs.at[there], single.at[zi], ob_sem.at[6], ob_sem.at[7], z_peer(d))
        for d, slot in ((1, 0), (nz - 1, 2)):
            source = obs.at[double_at(d, 0, double)]
            send(source, near.at[slot], ob_sem.at[4], ob_sem.at[5], z_peer(d))

    landed(obs, load_sem.at[6 + variables])
    @pl.when(ci != lead)
    def _():
        obs_copies()

    landed(innov, load_sem.at[2])
    landed(valid, load_sem.at[3])
    landed(types, load_sem.at[4])
    landed(inverse, load_sem.at[5])
    eye = iota((slots, slots), 0) == iota((slots, slots), 1)

    def column(line):
        wide = jnp.broadcast_to(line.astype(F32), (slots, slots))
        return jnp.sum(jnp.where(eye, wide, 0.0), axis=1, keepdims=True)

    type_col = column(types[...])
    valid_col = column(valid[...])
    inverse_col = jnp.zeros((slots, 1), F32)
    for c in range(NTYPES):
        inverse_col = jnp.where(type_col == c, inverse[0:1, c : c + 1], inverse_col)
    inside = iota((slots, rows), 1).astype(F32) < valid_col
    scal[...] = innov[...] * inverse_col * inside.astype(F32) / member_scale
    onehot = (iota((NTYPES, slots), 0) == types[...]).astype(BF16)
    onehot = jnp.concatenate([onehot, onehot], axis=1)
    g_add = jnp.zeros((4, 128), F32)
    for m in range(members):
        prod = obs[:, m].astype(F32).reshape(slots, rows) * scal[...]
        high = prod.astype(BF16)
        low = (prod - high.astype(F32)).astype(BF16)
        by_type = jnp.dot(
            onehot, jnp.concatenate([high, low], axis=0), preferred_element_type=F32
        )
        g = jnp.sum(by_type, axis=1, keepdims=True)
        g_add = jnp.where(lane4 == total_members + m, g[0:4], g_add)
        g_add = jnp.where(lane4 == total_members + members + m, g[4:8], g_add)
    sums_src[1] = g_add

    def g_copy():
        return remote(
            sums_src.at[1], g_in.at[0], g_sem.at[0], g_sem.at[1], {"lat_2": other_core}
        )

    @pl.when(ci != lead)
    def _():
        g_copy().start()

    my_class = lax.rem(zi, owners)
    near[1] = obs[pl.ds(my_class * double, double)]
    if n_single:
        single[pl.ds(zi, 1)] = obs[pl.ds(single_base + zi * n_single, n_single)][None]

    width = 4 * one
    pitch = -(-width // 128) * 128
    spot = iota((128, pitch), 1)

    def select(first):
        wanted = lax.rem(
            (zi + nz + first) * members + spot // eight, total_members
        )
        return ((iota((128, pitch), 0) == wanted) & (spot < width)).astype(BF16)

    tables = [select(-1), select(-2)]
    if n_single:
        shape = (128, nz * one)
        tables.append((iota(shape, 0) == iota(shape, 1) // eight).astype(BF16))
    sel = jnp.concatenate(tables, axis=1)
    row_t = iota((targets * eight, targets), 0) // eight
    spread = (
        iota((targets * eight, targets), 1)
        == lax.rem(row_t, REGIONS) * variables + row_t // REGIONS
    ).astype(BF16)
    sel_own = (
        (iota((128, 128), 0) == iota((128, 128), 1) + zi * members)
        & (iota((128, 128), 1) < members)
    ).astype(BF16)
    perm_r = iota((targets, targets), 0)
    perm = (
        iota((targets, targets), 1) == lax.rem(perm_r, REGIONS) * variables + perm_r // REGIONS
    ).astype(BF16)

    def y_copy(d):
        return remote(
            sums_src.at[2], my.at[yi], my_sem.at[0], my_sem.at[1], y_peer(d)
        )

    def x_copy(d, core):
        return remote(
            sums_src.at[3],
            mx.at[xi],
            mx_sem.at[0],
            mx_sem.at[1],
            x_peer(d, core),
        )

    @pl.when(ci == lead)
    def _():
        g_copy().wait_recv()
        landed(mz.at[pl.ds(0, nz * nc - 1)], mz_sem.at[1])
        total = mz[0]
        for z in range(1, nz * nc):
            total = total + mz[z]
        total = total + g_add + g_in[0]
        sums_src[2] = total
        my[pl.ds(yi, 1)] = total[None]
        for d in ring_order(ny):
            y_copy(d).start()

    @pl.when(ci == lead)
    def _():
        obs_copies()

    @pl.when(ci == lead)
    def _():
        landed(my.at[pl.ds(0, ny - 1)], my_sem.at[1])
        total = my[0]
        for y in range(1, ny):
            total = total + my[y]
        sums_src[3] = total
        mx[pl.ds(xi, 1)] = total[None]
        for d in ring_order(nx) + [0]:
            for core in range(nc):
                if d or core != lead:
                    x_copy(d, core).start()

    if n_down:
        landed(far_down, ob_sem.at[1])
    if n_up:
        landed(far_up, ob_sem.at[3])
    landed(near.at[pl.ds(0, 2)], ob_sem.at[5])
    if n_single:
        landed(single.at[pl.ds(0, nz - 1)], ob_sem.at[7])

    def rows_of(value):
        return value.astype(F32).reshape(-1, rows).astype(BF16)

    for p in range(double):
        close = rows_of(near[:, p])
        if p < n_up:
            packed[p, 0 : 3 * one, :] = close
            packed[p, 3 * one : width, :] = rows_of(far_up[p])
        else:
            packed[p, one:width, :] = close
            packed[p, 0:one, :] = rows_of(far_down[p - n_up])
    for p in range(n_single):
        packed_single[p] = rows_of(single[:, p])

    @pl.when(ci == lead)
    def _():
        landed(mx.at[pl.ds(0, nx - 1)], mx_sem.at[1])

    @pl.when(ci != lead)
    def _():
        landed(mx, mx_sem.at[1])

    sums = jnp.concatenate([mx[x] for x in range(nx)], axis=0)
    lane16 = iota((targets, 128), 1)
    w = jnp.where(lane16 < total_members, sums / norm_scale, 0.0).astype(BF16)
    wide = jnp.dot(w, sel, preferred_element_type=F32).astype(BF16)
    tall = jnp.dot(spread, wide, preferred_element_type=F32)
    keep = lax.rem(iota(tall.shape, 0), eight) == lax.rem(iota(tall.shape, 1), eight)
    wd = jnp.where(keep, tall, 0.0).astype(BF16)

    def respond(pieces_here):
        for p in pieces_here:
            if p < double:
                first = 0 if p < n_up else pitch
                answered = jnp.dot(
                    wd[:, first : first + width], packed[p], preferred_element_type=F32
                )
            else:
                answered = jnp.dot(
                    wd[:, 2 * pitch :], packed_single[p - double], preferred_element_type=F32
                )
            resp_src[:, p] = answered.astype(BF16).reshape(nz, pair * eight, rows)
            if p != double - 1 and p != pieces - 1:
                continue
            first = 0 if p < double else double
            ready = pl.ds(first, p + 1 - first)
            for d in ring_order(nz):
                send(
                    resp_src.at[lax.rem(zi + d, nz), ready],
                    resp_in.at[zi, ready],
                    rs_sem.at[2],
                    rs_sem.at[first // double],
                    z_peer(d),
                )

    respond(range(double))

    g_all = mx[0]
    for x in range(1, nx):
        g_all = g_all + mx[x]
    w_own = jnp.dot(w, sel_own, preferred_element_type=F32).astype(BF16)
    w_own = jnp.dot(perm, w_own, preferred_element_type=F32)
    g_rows = jnp.concatenate(
        [
            pltpu.roll(g_all, 128 - total_members, 1),
            pltpu.roll(g_all, 128 - total_members - members, 1),
        ],
        axis=0,
    )
    g_rows = jnp.where(iota((NTYPES, 128), 1) < members, g_rows, 0.0)
    share = jnp.zeros((targets, 128), F32)
    for c in range(NTYPES):
        col = jnp.sum(w_own * g_rows[c : c + 1], axis=1, keepdims=True)
        share = jnp.where(lane16 == c, col, share)
    for z in range(nz):
        pt_src[z, 0:pair, :] = share[pair * z : pair * z + pair]
    top = pl.ds(0, pair)
    for d in ring_order(nz):
        other = lax.rem(zi + d, nz)
        send(pt_src.at[other, top], pt_in.at[zi, top], pt_sem.at[0], pt_sem.at[1], z_peer(d))
    pt_in[pl.ds(zi, 1), 0:pair, :] = pt_src[pl.ds(zi, 1), 0:pair, :]

    respond(range(double, pieces))
    resp_in[pl.ds(zi, 1)] = resp_src[pl.ds(zi, 1)]

    def place(value, group):
        start = group * eight
        for t in range(pair):
            line = value[t * eight : (t + 1) * eight] * scal[start : start + eight, :]
            for lane in range(rows // 128):
                spot = (start * (rows // 128) + lane) * pair + t
                out_ref[pl.ds(spot, eight, stride=pair * (rows // 128)), :] = line[
                    :, lane * 128 : (lane + 1) * 128
                ]

    for p in range(pieces):
        if p == 0:
            landed(resp_in.at[pl.ds(0, nz - 1), pl.ds(0, double)], rs_sem.at[0])
        elif p == double:
            landed(resp_in.at[pl.ds(0, nz - 1), pl.ds(double, n_single)], rs_sem.at[1])
        if p < double:
            for c in range(owners):
                value = resp_in[c, p].astype(F32) + resp_in[c + owners, p].astype(F32)
                place(value, c * double + p)
        else:
            for z in range(nz):
                place(resp_in[z, p].astype(F32), single_base + z * n_single + p - double)
    landed(pt_in.at[pl.ds(0, nz - 1), top], pt_sem.at[1])
    whole = pt_in[0, 0:pair, :]
    for z in range(1, nz):
        whole = whole + pt_in[z, 0:pair, :]
    tot_ref[...] = whole[:, 0:NTYPES] / total_scale

    if n_down:
        landed(far_down, ob_sem.at[0])
    if n_up:
        landed(far_up, ob_sem.at[2])
    landed(near.at[pl.ds(0, 2)], ob_sem.at[4])
    if n_single:
        landed(single.at[pl.ds(0, nz - 1)], ob_sem.at[6])
    landed(resp_src.at[pl.ds(0, nz - 1)], rs_sem.at[2])
    landed(pt_src.at[pl.ds(0, nz - 1), top], pt_sem.at[0])

    @pl.when(ci != lead)
    def _():
        landed(mz.at[pl.ds(0, nz)], mz_sem.at[0])
        g_copy().wait_send()

    @pl.when(ci == lead)
    def _():
        landed(mz.at[pl.ds(0, nz - 1)], mz_sem.at[0])
        landed(my.at[pl.ds(0, ny - 1)], my_sem.at[0])
        landed(mz.at[pl.ds(0, nx * nc - 1)], mx_sem.at[0])


def store_kernel(out_ref, tot_ref, out_hbm, tot_hbm, sems):
    copies = [
        pltpu.make_async_copy(out_ref, out_hbm, sems.at[0]),
        pltpu.make_async_copy(tot_ref, tot_hbm, sems.at[1]),
    ]
    for copy in copies:
        copy.start()
    for copy in copies:
        copy.wait()


def local(
    anomalies,
    error_now,
    error_prior,
    energy_coef,
    obs_anomalies,
    innovations,
    valid_counts,
    type_ids,
    error_inverse,
):
    dims = tuple(lax.axis_size(a) for a in (*LAT, "lev"))
    nx, ny, nc, nz = dims
    variables, levels, members, lat_rows, lon_count = anomalies.shape
    slots, local_members, rows = obs_anomalies.shape
    lat_total = lat_rows * nx * ny * nc
    norm_scale = math.sqrt(levels * nz * lat_total * lon_count / REGIONS)
    member_scale = math.sqrt(members - 1)
    total_scale = math.sqrt(slots * nx * ny * nc * rows / NTYPES)
    targets = variables * REGIONS
    pair = targets // nz
    n_up, n_down, n_single = SHARES
    double = n_up + n_down
    pieces = double + n_single
    tiles = lon_count // 128 * lat_rows

    def by_tile(a):
        a = a.reshape(*a.shape[:-1], lon_count // 128, 128)
        n = a.ndim
        order = (*range(n - 3), n - 2, n - 3, n - 1)
        a = with_layout_constraint(a, Layout(major_to_minor=order))
        a = jnp.swapaxes(a, -3, -2)
        return a.reshape(*a.shape[:-3], tiles, 128)

    anom = by_tile(anomalies[:, 0]).reshape(variables, members // 2, 2 * tiles, 128)
    now = by_tile(error_now[:, 0])
    prior = by_tile(error_prior[:, 0])
    obs = jnp.transpose(obs_anomalies, (1, 0, 2)).reshape(local_members, slots // 8, 8, rows)
    inputs = (
        anom,
        now,
        prior,
        energy_coef.reshape(1, variables),
        obs,
        innovations,
        valid_counts.reshape(1, slots),
        type_ids.reshape(1, slots),
        error_inverse.reshape(1, NTYPES),
    )
    vmem = pl.BlockSpec(memory_space=pltpu.VMEM)
    hbm = pl.BlockSpec(memory_space=pltpu.HBM)
    dma = pltpu.SemaphoreType.DMA
    table = pltpu.VMEM
    out, totals = pl.pallas_call(
        functools.partial(
            exchange_kernel,
            dims,
            (variables, members, lat_rows),
            SHARES,
            norm_scale,
            member_scale,
            total_scale,
        ),
        out_shape=(
            jax.ShapeDtypeStruct((slots * pair * rows // 128, 128), F32),
            jax.ShapeDtypeStruct((pair, NTYPES), F32),
        ),
        in_specs=[hbm] * len(inputs),
        out_specs=(vmem, vmem),
        scratch_shapes=[
            table(anom.shape, BF16),
            table((2, *now.shape), F32),
            table((1, variables), F32),
            table((slots // 8, local_members, 8, rows), BF16),
            table((slots, rows), F32),
            table((1, slots), jnp.int32),
            table((1, slots), jnp.int32),
            table((1, NTYPES), F32),
        ]
        + [
            table((variables, members * 8, 128), F32),
            table((slots, rows), F32),
            table((nz * nc, 4, 128), F32),
            table((ny, 4, 128), F32),
            table((nx, 4, 128), F32),
            table((4, 4, 128), F32),
            table((1, 4, 128), F32),
            table((3, double, local_members, 8, rows), BF16),
            table((max(n_up, 1), local_members, 8, rows), BF16),
            table((max(n_down, 1), local_members, 8, rows), BF16),
            table((nz, max(n_single, 1), local_members, 8, rows), BF16),
            table((double, 32 * local_members, rows), BF16),
            table((max(n_single, 1), 8 * nz * local_members, rows), BF16),
            table((nz, pieces, pair * 8, rows), BF16),
            table((nz, pieces, pair * 8, rows), BF16),
            table((nz, 8, 128), F32),
            table((nz, 8, 128), F32),
            dma((7 + variables,)),
            dma((2,)),
            dma((2,)),
            dma((2,)),
            dma((2,)),
            dma((8,)),
            dma((3,)),
            dma((2,)),
        ],
        compiler_params=pltpu.CompilerParams(
            collective_id=0, has_side_effects=True, vmem_limit_bytes=24 * 1024 * 1024
        ),
    )(*(pltpu.with_memory_space_constraint(a, pltpu.HBM) for a in inputs))
    out, totals = pl.pallas_call(
        store_kernel,
        out_shape=(pltpu.HBM(out.shape, F32), pltpu.HBM(totals.shape, F32)),
        in_specs=[vmem, vmem],
        out_specs=(hbm, hbm),
        scratch_shapes=[dma((2,))],
        compiler_params=pltpu.CompilerParams(vmem_limit_bytes=4 * 1024 * 1024),
    )(out, totals)
    impact = out.reshape(slots, rows // 128, pair, 128)
    impact = jnp.transpose(impact, (0, 2, 1, 3)).reshape(slots, pair, rows)
    return (impact, totals)


def solution(mesh):
    split = Mesh(
        mesh.devices.reshape(4, 8, 2, mesh.shape["lev"]), ("lat_0", "lat_1", "lat_2", "lev")
    )
    in_specs = (
        P(None, "lev", None, LAT, None),
        P(None, "lev", LAT, None),
        P(None, "lev", LAT, None),
        P(None, "lev"),
        P(LAT, "lev", None),
        P(LAT, None),
        P(LAT),
        P(LAT),
        P(),
    )
    out_specs = (P(LAT, "lev", None), P("lev", None))
    return jax.shard_map(local, mesh=split, in_specs=in_specs, out_specs=out_specs, check_vma=False)
```

```python
import functools
import math

import jax
import jax.numpy as jnp
from jax import lax
from jax.experimental.layout import Layout, with_layout_constraint
from jax.experimental import pallas as pl
from jax.experimental.pallas import tpu as pltpu
from jax.sharding import Mesh
from jax.sharding import PartitionSpec as P

NLAT_GRID = 768
LAT0 = 256
REGIONS = 4
NTYPES = 8
LAT = ("lat_0", "lat_1", "lat_2")
MESH = pl.DeviceIdType.MESH
EARLY = True
SHARES = (2, 0, 1)
F32 = jnp.float32
BF16 = jnp.bfloat16


def ring_order(n):
    return sorted(range(1, n), key=lambda d: (-min(d, n - d), d))


def exchange_kernel(
    dims,
    counts,
    shares,
    norm_scale,
    member_scale,
    total_scale,
    anom_ref,
    now_ref,
    prior_ref,
    energy_ref,
    obs_ref,
    innov_ref,
    valid_ref,
    type_ref,
    inverse_ref,
    out_ref,
    tot_ref,
    anom,
    errors,
    energy,
    obs,
    innov,
    valid,
    types,
    inverse,
    folded,
    scal,
    mz,
    my,
    mx,
    sums_src,
    g_in,
    near,
    far_up,
    far_down,
    single,
    packed,
    packed_single,
    resp_src,
    resp_in,
    pt_src,
    pt_in,
    load_sem,
    mz_sem,
    g_sem,
    my_sem,
    mx_sem,
    ob_sem,
    rs_sem,
    pt_sem,
):
    nx, ny, nc, nz = dims
    variables, total_members, lat_rows = counts
    n_up, n_down, n_single = shares
    groups, members, eight, rows = obs.shape
    slots = groups * eight
    owners = nz // 2
    double = n_up + n_down
    single_base = owners * double
    pieces = double + n_single
    targets = variables * REGIONS
    pair = targets // nz
    lon_tiles = errors.shape[2]
    one = members * eight
    xi = lax.axis_index("lat_0")
    yi = lax.axis_index("lat_1")
    ci = lax.axis_index("lat_2")
    zi = lax.axis_index("lev")
    lead = nc - 1

    def z_peer(d, core=None):
        peer = {"lev": lax.rem(zi + d, nz)}
        if core is not None:
            peer["lat_2"] = core
        return peer

    def x_peer(d, core=None):
        peer = {"lat_0": lax.rem(xi + d, nx)}
        if core is not None:
            peer["lat_2"] = core
        return peer

    def y_peer(d):
        return {"lat_1": lax.rem(yi + d, ny)}

    def remote(source, target, send_sem, recv_sem, peer):
        return pltpu.make_async_remote_copy(
            src_ref=source,
            dst_ref=target,
            send_sem=send_sem,
            recv_sem=recv_sem,
            device_id=peer,
            device_id_type=MESH,
        )

    def send(source, target, send_sem, recv_sem, peer):
        remote(source, target, send_sem, recv_sem, peer).start()

    def iota(shape, axis):
        return lax.broadcasted_iota(jnp.int32, shape, axis)

    barrier = pltpu.get_barrier_semaphore()
    other_core = nc - 1 - ci
    partner = {"lat_2": other_core}

    def greet(hops):
        for _, peer in sorted(hops, key=lambda h: -h[0]):
            pl.semaphore_signal(barrier, inc=1, device_id=peer, device_id_type=MESH)

    def far(d, n):
        return min(d, n - d)

    z_same = [(far(d, nz), z_peer(d)) for d in ring_order(nz)]
    x_lead = [(far(d, nx), x_peer(d, lead)) for d in ring_order(nx)]

    @pl.when(ci == lead)
    def _():
        z_other = [(far(d, nz), z_peer(d, other_core)) for d in ring_order(nz)]
        along_y = [(far(d, ny), y_peer(d)) for d in ring_order(ny)]
        greet(z_same + z_other + along_y + x_lead + [(0, partner)])

    @pl.when(ci != lead)
    def _():
        greet(z_same + x_lead + [(0, partner)])

    def load(source, target, n):
        pltpu.make_async_copy(source, target, load_sem.at[n]).start()

    def landed(target, sem):
        pltpu.make_async_copy(target, target, sem).wait()

    load(now_ref, errors.at[0], 0)
    load(prior_ref, errors.at[1], 0)
    load(energy_ref, energy, 1)
    for v in range(0, variables, 2):
        load(anom_ref.at[pl.ds(v, 2)], anom.at[pl.ds(v, 2)], 6 + v // 2)
    for m in range(members):
        load(obs_ref.at[m], obs.at[:, m], 6 + variables // 2)
    load(innov_ref, innov, 2)
    load(valid_ref, valid, 3)
    load(type_ref, types, 4)
    load(inverse_ref, inverse, 5)

    lat_index = ((xi * ny + yi) * nc + ci) * lat_rows + lax.rem(
        iota((lon_tiles, 128), 0), lat_rows
    )
    cosine = jnp.cos(
        -0.5 * math.pi + ((lat_index + LAT0).astype(F32) + 0.5) * math.pi / NLAT_GRID
    )
    landed(errors, load_sem.at[0])
    landed(energy, load_sem.at[1])
    for v in range(variables):
        grad = energy[0:1, v : v + 1] * cosine * (errors[0, v] + errors[1, v])
        grad = grad.astype(BF16).astype(F32)
        if v % 2 == 0:
            landed(anom.at[pl.ds(v, 2)], load_sem.at[6 + v // 2])
        step = 4
        for k in range(0, anom.shape[1], step):
            a = anom[v, k : k + step].astype(F32)
            a = a.reshape(-1, lon_tiles, 128) * grad[None]
            a = a.reshape(a.shape[0], lon_tiles // 8, 8, 128).sum(axis=1)
            folded[v, k * 16 : (k + step) * 16, :] = a.reshape(-1, 128)
    lane80 = iota((total_members, 128), 1)
    flat = jnp.zeros((total_members, 128), F32)
    for v in range(variables):
        s = folded[v, pl.ds(0, total_members, stride=8), :]
        for r in range(1, 8):
            s = s + folded[v, pl.ds(r, total_members, stride=8), :]
        flat = jnp.where(lane80 == v, jnp.sum(s, axis=1, keepdims=True), flat)
    flat = jnp.concatenate([flat, jnp.zeros((128 - total_members, 128), F32)], axis=0)
    base = jnp.transpose(flat)[0:4]
    lane4 = iota((4, 128), 1)
    sums_src[0] = base
    here_z = zi * nc + ci
    mz[pl.ds(here_z, 1)] = base[None]

    def z_copy(d):
        return remote(
            sums_src.at[0],
            mz.at[here_z],
            mz_sem.at[0],
            mz_sem.at[1],
            z_peer(d, lead),
        )

    @pl.when(ci == lead)
    def _():
        pl.semaphore_wait(barrier, nz - 1 + ny - 1 + nc * (nx - 1) + 1)

    @pl.when(ci != lead)
    def _():
        pl.semaphore_wait(barrier, nc * (nz - 1) + 1)

    for d in ring_order(nz):
        z_copy(d).start()

    @pl.when(ci != lead)
    def _():
        z_copy(0).start()

    def obs_copies():
        def double_at(d, first, size):
            c = lax.rem(zi + d, owners)
            return pl.ds(c * double + first, size)

        far = nz - 2
        if n_down:
            send(obs.at[double_at(2, n_up, n_down)], far_down, ob_sem.at[0], ob_sem.at[1], z_peer(2))
        if n_up:
            send(obs.at[double_at(far, 0, n_up)], far_up, ob_sem.at[2], ob_sem.at[3], z_peer(far))
        if n_single:
            for d in ring_order(nz):
                there = pl.ds(single_base + lax.rem(zi + d, nz) * n_single, n_single)
                send(obs.at[there], single.at[zi], ob_sem.at[6], ob_sem.at[7], z_peer(d))
        for d, slot in ((1, 0), (nz - 1, 2)):
            source = obs.at[double_at(d, 0, double)]
            send(source, near.at[slot], ob_sem.at[4], ob_sem.at[5], z_peer(d))

    landed(obs, load_sem.at[6 + variables // 2])
    @pl.when(ci != lead)
    def _():
        obs_copies()

    landed(innov, load_sem.at[2])
    landed(valid, load_sem.at[3])
    landed(types, load_sem.at[4])
    landed(inverse, load_sem.at[5])
    eye = iota((slots, slots), 0) == iota((slots, slots), 1)

    def column(line):
        wide = jnp.broadcast_to(line.astype(F32), (slots, slots))
        return jnp.sum(jnp.where(eye, wide, 0.0), axis=1, keepdims=True)

    type_col = column(types[...])
    valid_col = column(valid[...])
    inverse_col = jnp.zeros((slots, 1), F32)
    for c in range(NTYPES):
        inverse_col = jnp.where(type_col == c, inverse[0:1, c : c + 1], inverse_col)
    inside = iota((slots, rows), 1).astype(F32) < valid_col
    scal[...] = innov[...] * inverse_col * inside.astype(F32) / member_scale
    onehot = (iota((NTYPES, slots), 0) == types[...]).astype(BF16)
    onehot = jnp.concatenate([onehot, onehot], axis=1)
    g_add = jnp.zeros((4, 128), F32)
    for m in range(members):
        prod = obs[:, m].astype(F32).reshape(slots, rows) * scal[...]
        high = prod.astype(BF16)
        low = (prod - high.astype(F32)).astype(BF16)
        by_type = jnp.dot(
            onehot, jnp.concatenate([high, low], axis=0), preferred_element_type=F32
        )
        g = jnp.sum(by_type, axis=1, keepdims=True)
        g_add = jnp.where(lane4 == total_members + m, g[0:4], g_add)
        g_add = jnp.where(lane4 == total_members + members + m, g[4:8], g_add)
    sums_src[1] = g_add

    def g_copy():
        return remote(
            sums_src.at[1], g_in.at[0], g_sem.at[0], g_sem.at[1], {"lat_2": other_core}
        )

    @pl.when(ci != lead)
    def _():
        g_copy().start()

    my_class = lax.rem(zi, owners)
    near[1] = obs[pl.ds(my_class * double, double)]
    if n_single:
        single[pl.ds(zi, 1)] = obs[pl.ds(single_base + zi * n_single, n_single)][None]

    width = 4 * one
    pitch = -(-width // 128) * 128
    spot = iota((128, pitch), 1)

    def select(first):
        wanted = lax.rem(
            (zi + nz + first) * members + spot // eight, total_members
        )
        return ((iota((128, pitch), 0) == wanted) & (spot < width)).astype(BF16)

    tables = ([select(-1)] if n_up else []) + ([select(-2)] if n_down else [])
    doubles = len(tables)
    if n_single:
        shape = (128, nz * one)
        tables.append((iota(shape, 0) == iota(shape, 1) // eight).astype(BF16))
    sel = jnp.concatenate(tables, axis=1)
    row_t = iota((targets * eight, targets), 0) // eight
    spread = (
        iota((targets * eight, targets), 1)
        == lax.rem(row_t, REGIONS) * variables + row_t // REGIONS
    ).astype(BF16)
    sel_own = (
        (iota((128, 128), 0) == iota((128, 128), 1) + zi * members)
        & (iota((128, 128), 1) < members)
    ).astype(BF16)
    perm_r = iota((targets, targets), 0)
    perm = (
        iota((targets, targets), 1) == lax.rem(perm_r, REGIONS) * variables + perm_r // REGIONS
    ).astype(BF16)

    def y_copy(d):
        return remote(
            sums_src.at[2], my.at[yi], my_sem.at[0], my_sem.at[1], y_peer(d)
        )

    def x_copy(d, core):
        return remote(
            sums_src.at[3],
            mx.at[xi],
            mx_sem.at[0],
            mx_sem.at[1],
            x_peer(d, core),
        )

    @pl.when(ci == lead)
    def _():
        g_copy().wait_recv()
        landed(mz.at[pl.ds(0, nz * nc - 1)], mz_sem.at[1])
        total = mz[0]
        for z in range(1, nz * nc):
            total = total + mz[z]
        total = total + g_add + g_in[0]
        sums_src[2] = total
        my[pl.ds(yi, 1)] = total[None]
        for d in ring_order(ny):
            y_copy(d).start()

    @pl.when(ci == lead)
    def _():
        obs_copies()

    @pl.when(ci == lead)
    def _():
        landed(my.at[pl.ds(0, ny - 1)], my_sem.at[1])
        total = my[0]
        for y in range(1, ny):
            total = total + my[y]
        sums_src[3] = total
        mx[pl.ds(xi, 1)] = total[None]
        for d in ring_order(nx) + [0]:
            for core in range(nc):
                if d or core != lead:
                    x_copy(d, core).start()

    if n_down:
        landed(far_down, ob_sem.at[1])
    if n_up:
        landed(far_up, ob_sem.at[3])
    landed(near.at[pl.ds(0, 2)], ob_sem.at[5])
    if n_single:
        landed(single.at[pl.ds(0, nz - 1)], ob_sem.at[7])

    def rows_of(value):
        return value.astype(F32).reshape(-1, rows).astype(BF16)

    for p in range(double):
        close = rows_of(near[:, p])
        if p < n_up:
            packed[p, 0 : 3 * one, :] = close
            packed[p, 3 * one : width, :] = rows_of(far_up[p])
        else:
            packed[p, one:width, :] = close
            packed[p, 0:one, :] = rows_of(far_down[p - n_up])
    for p in range(n_single):
        packed_single[p] = rows_of(single[:, p])

    @pl.when(ci == lead)
    def _():
        landed(mx.at[pl.ds(0, nx - 1)], mx_sem.at[1])

    @pl.when(ci != lead)
    def _():
        landed(mx, mx_sem.at[1])

    sums = jnp.concatenate([mx[x] for x in range(nx)], axis=0)
    lane16 = iota((targets, 128), 1)
    w = jnp.where(lane16 < total_members, sums / norm_scale, 0.0).astype(BF16)
    wide = jnp.dot(w, sel, preferred_element_type=F32).astype(BF16)
    tall = jnp.dot(spread, wide, preferred_element_type=F32)
    keep = lax.rem(iota(tall.shape, 0), eight) == lax.rem(iota(tall.shape, 1), eight)
    wd = jnp.where(keep, tall, 0.0).astype(BF16)

    def respond(pieces_here):
        for p in pieces_here:
            if p < double:
                first = 0 if p < n_up or doubles == 1 else pitch
                answered = jnp.dot(
                    wd[:, first : first + width], packed[p], preferred_element_type=F32
                )
            else:
                answered = jnp.dot(
                    wd[:, doubles * pitch :], packed_single[p - double], preferred_element_type=F32
                )
            resp_src[:, p] = answered.astype(BF16).reshape(nz, pair * eight, rows)
            if p != double - 1 and p != pieces - 1:
                continue
            first = 0 if p < double else double
            ready = pl.ds(first, p + 1 - first)
            for d in ring_order(nz):
                send(
                    resp_src.at[lax.rem(zi + d, nz), ready],
                    resp_in.at[zi, ready],
                    rs_sem.at[2],
                    rs_sem.at[first // double],
                    z_peer(d),
                )

    respond(range(double))

    g_all = mx[0]
    for x in range(1, nx):
        g_all = g_all + mx[x]
    w_own = jnp.dot(w, sel_own, preferred_element_type=F32).astype(BF16)
    w_own = jnp.dot(perm, w_own, preferred_element_type=F32)
    g_rows = jnp.concatenate(
        [
            pltpu.roll(g_all, 128 - total_members, 1),
            pltpu.roll(g_all, 128 - total_members - members, 1),
        ],
        axis=0,
    )
    g_rows = jnp.where(iota((NTYPES, 128), 1) < members, g_rows, 0.0)
    share = jnp.zeros((targets, 128), F32)
    for c in range(NTYPES):
        col = jnp.sum(w_own * g_rows[c : c + 1], axis=1, keepdims=True)
        share = jnp.where(lane16 == c, col, share)
    for z in range(nz):
        pt_src[z, 0:pair, :] = share[pair * z : pair * z + pair]
    top = pl.ds(0, pair)
    for d in ring_order(nz):
        other = lax.rem(zi + d, nz)
        send(pt_src.at[other, top], pt_in.at[zi, top], pt_sem.at[0], pt_sem.at[1], z_peer(d))
    pt_in[pl.ds(zi, 1), 0:pair, :] = pt_src[pl.ds(zi, 1), 0:pair, :]

    respond(range(double, pieces))
    resp_in[pl.ds(zi, 1)] = resp_src[pl.ds(zi, 1)]

    def place(value, group):
        start = group * eight
        for t in range(pair):
            line = value[t * eight : (t + 1) * eight] * scal[start : start + eight, :]
            for lane in range(rows // 128):
                spot = (start * (rows // 128) + lane) * pair + t
                out_ref[pl.ds(spot, eight, stride=pair * (rows // 128)), :] = line[
                    :, lane * 128 : (lane + 1) * 128
                ]

    for p in range(pieces):
        if p == 0:
            landed(resp_in.at[pl.ds(0, nz - 1), pl.ds(0, double)], rs_sem.at[0])
        elif p == double:
            landed(resp_in.at[pl.ds(0, nz - 1), pl.ds(double, n_single)], rs_sem.at[1])
        if p < double:
            for c in range(owners):
                value = resp_in[c, p].astype(F32) + resp_in[c + owners, p].astype(F32)
                place(value, c * double + p)
        else:
            for z in range(nz):
                place(resp_in[z, p].astype(F32), single_base + z * n_single + p - double)
    landed(pt_in.at[pl.ds(0, nz - 1), top], pt_sem.at[1])
    whole = pt_in[0, 0:pair, :]
    for z in range(1, nz):
        whole = whole + pt_in[z, 0:pair, :]
    tot_ref[...] = whole[:, 0:NTYPES] / total_scale

    if n_down:
        landed(far_down, ob_sem.at[0])
    if n_up:
        landed(far_up, ob_sem.at[2])
    landed(near.at[pl.ds(0, 2)], ob_sem.at[4])
    if n_single:
        landed(single.at[pl.ds(0, nz - 1)], ob_sem.at[6])
    landed(resp_src.at[pl.ds(0, nz - 1)], rs_sem.at[2])
    landed(pt_src.at[pl.ds(0, nz - 1), top], pt_sem.at[0])

    @pl.when(ci != lead)
    def _():
        landed(mz.at[pl.ds(0, nz)], mz_sem.at[0])
        g_copy().wait_send()

    @pl.when(ci == lead)
    def _():
        landed(mz.at[pl.ds(0, nz - 1)], mz_sem.at[0])
        landed(my.at[pl.ds(0, ny - 1)], my_sem.at[0])
        landed(mz.at[pl.ds(0, nx * nc - 1)], mx_sem.at[0])


def store_kernel(out_ref, tot_ref, out_hbm, tot_hbm, sems):
    copies = [
        pltpu.make_async_copy(out_ref, out_hbm, sems.at[0]),
        pltpu.make_async_copy(tot_ref, tot_hbm, sems.at[1]),
    ]
    for copy in copies:
        copy.start()
    for copy in copies:
        copy.wait()


def local(
    anomalies,
    error_now,
    error_prior,
    energy_coef,
    obs_anomalies,
    innovations,
    valid_counts,
    type_ids,
    error_inverse,
):
    dims = tuple(lax.axis_size(a) for a in (*LAT, "lev"))
    nx, ny, nc, nz = dims
    variables, levels, members, lat_rows, lon_count = anomalies.shape
    slots, local_members, rows = obs_anomalies.shape
    lat_total = lat_rows * nx * ny * nc
    norm_scale = math.sqrt(levels * nz * lat_total * lon_count / REGIONS)
    member_scale = math.sqrt(members - 1)
    total_scale = math.sqrt(slots * nx * ny * nc * rows / NTYPES)
    targets = variables * REGIONS
    pair = targets // nz
    n_up, n_down, n_single = SHARES
    double = n_up + n_down
    pieces = double + n_single
    tiles = lon_count // 128 * lat_rows

    def by_tile(a):
        a = a.reshape(*a.shape[:-1], lon_count // 128, 128)
        n = a.ndim
        order = (*range(n - 3), n - 2, n - 3, n - 1)
        a = with_layout_constraint(a, Layout(major_to_minor=order))
        a = jnp.swapaxes(a, -3, -2)
        return a.reshape(*a.shape[:-3], tiles, 128)

    anom = by_tile(anomalies[:, 0]).reshape(variables, members // 2, 2 * tiles, 128)
    now = by_tile(error_now[:, 0])
    prior = by_tile(error_prior[:, 0])
    obs = jnp.transpose(obs_anomalies, (1, 0, 2)).reshape(local_members, slots // 8, 8, rows)
    inputs = (
        anom,
        now,
        prior,
        energy_coef.reshape(1, variables),
        obs,
        innovations,
        valid_counts.reshape(1, slots),
        type_ids.reshape(1, slots),
        error_inverse.reshape(1, NTYPES),
    )
    vmem = pl.BlockSpec(memory_space=pltpu.VMEM)
    hbm = pl.BlockSpec(memory_space=pltpu.HBM)
    dma = pltpu.SemaphoreType.DMA
    table = pltpu.VMEM
    out, totals = pl.pallas_call(
        functools.partial(
            exchange_kernel,
            dims,
            (variables, members, lat_rows),
            SHARES,
            norm_scale,
            member_scale,
            total_scale,
        ),
        out_shape=(
            jax.ShapeDtypeStruct((slots * pair * rows // 128, 128), F32),
            jax.ShapeDtypeStruct((pair, NTYPES), F32),
        ),
        in_specs=[hbm] * len(inputs),
        out_specs=(vmem, vmem),
        scratch_shapes=[
            table(anom.shape, BF16),
            table((2, *now.shape), F32),
            table((1, variables), F32),
            table((slots // 8, local_members, 8, rows), BF16),
            table((slots, rows), F32),
            table((1, slots), jnp.int32),
            table((1, slots), jnp.int32),
            table((1, NTYPES), F32),
        ]
        + [
            table((variables, members * 8, 128), F32),
            table((slots, rows), F32),
            table((nz * nc, 4, 128), F32),
            table((ny, 4, 128), F32),
            table((nx, 4, 128), F32),
            table((4, 4, 128), F32),
            table((1, 4, 128), F32),
            table((3, double, local_members, 8, rows), BF16),
            table((max(n_up, 1), local_members, 8, rows), BF16),
            table((max(n_down, 1), local_members, 8, rows), BF16),
            table((nz, max(n_single, 1), local_members, 8, rows), BF16),
            table((double, 32 * local_members, rows), BF16),
            table((max(n_single, 1), 8 * nz * local_members, rows), BF16),
            table((nz, pieces, pair * 8, rows), BF16),
            table((nz, pieces, pair * 8, rows), BF16),
            table((nz, 8, 128), F32),
            table((nz, 8, 128), F32),
            dma((7 + variables // 2,)),
            dma((2,)),
            dma((2,)),
            dma((2,)),
            dma((2,)),
            dma((8,)),
            dma((3,)),
            dma((2,)),
        ],
        compiler_params=pltpu.CompilerParams(
            collective_id=0, has_side_effects=True, vmem_limit_bytes=24 * 1024 * 1024
        ),
    )(*(pltpu.with_memory_space_constraint(a, pltpu.HBM) for a in inputs))
    out, totals = pl.pallas_call(
        store_kernel,
        out_shape=(pltpu.HBM(out.shape, F32), pltpu.HBM(totals.shape, F32)),
        in_specs=[vmem, vmem],
        out_specs=(hbm, hbm),
        scratch_shapes=[dma((2,))],
        compiler_params=pltpu.CompilerParams(vmem_limit_bytes=4 * 1024 * 1024),
    )(out, totals)
    impact = out.reshape(slots, rows // 128, pair, 128)
    impact = jnp.transpose(impact, (0, 2, 1, 3)).reshape(slots, pair, rows)
    return (impact, totals)


def solution(mesh):
    split = Mesh(
        mesh.devices.reshape(4, 8, 2, mesh.shape["lev"]), ("lat_0", "lat_1", "lat_2", "lev")
    )
    in_specs = (
        P(None, "lev", None, LAT, None),
        P(None, "lev", LAT, None),
        P(None, "lev", LAT, None),
        P(None, "lev"),
        P(LAT, "lev", None),
        P(LAT, None),
        P(LAT),
        P(LAT),
        P(),
    )
    out_specs = (P(LAT, "lev", None), P("lev", None))
    return jax.shard_map(local, mesh=split, in_specs=in_specs, out_specs=out_specs, check_vma=False)
```
